8 devices in a mesh: replica: 1 (over z), data2: 2 (over y), data: 4 (over x, core).
Axes of the slice: x: 2, y: 2, z: 1, core: 2. Of those that a mesh axis runs over, the one named last changes fastest.
Arguments:
- query_hidden: bfloat16 [128, 32, 1536], P(('replica', 'data2', 'data'))
- doc_hidden: bfloat16 [128, 768, 1536], P(('replica', 'data2', 'data'))
- w_proj: bfloat16 [1536, 128], replicated
- query_mask: int32 [128, 32], P(('replica', 'data2', 'data'))
- doc_mask: int32 [128, 768], P(('replica', 'data2', 'data'))
- temperature: float32 [], replicated
Outputs:
- output 1: float32 [128], P(('replica', 'data2', 'data'))
- output 2: float32 [1], P('replica')
All inputs are finite; a program needn't handle non-finite values.
Results may differ from the reference program's by a relative error of at most 0.001.
Values are sent between devices in bfloat16 or wider.
A program may use at most 1 GiB of HBM per device.

```python
import jax
import jax.numpy as jnp
from jax import lax

BATCH = 128
QLEN = 32
DLEN = 768
HIDDEN = 1536
PROJ = 128


def setup_inputs(seed: int = 0, part: int = 0) -> dict:
    root_key = jax.random.key(seed)
    key_common, key_parts = jax.random.split(root_key)
    part_key = jax.random.fold_in(key_parts, part)
    key_list = jax.random.split(part_key, 6)
    key_weight, key_temp = jax.random.split(key_common)
    shared = jax.random.normal(key_list[0], (HIDDEN,), jnp.float32)
    topic_vec = jax.random.normal(key_list[1], (BATCH, 1, HIDDEN), jnp.float32)
    concept = jax.random.normal(key_list[2], (BATCH, QLEN, HIDDEN), jnp.float32)
    token_noise = jax.random.normal(key_list[3], (BATCH, DLEN, HIDDEN), jnp.float32)
    query_lens = jax.random.randint(key_list[4], (BATCH,), QLEN // 2, QLEN + 1)
    doc_lens = jax.random.randint(key_list[5], (BATCH,), DLEN // 4, DLEN + 1)
    query_mask = (jnp.arange(QLEN)[None, :] < query_lens[:, None]).astype(jnp.int32)
    doc_mask = (jnp.arange(DLEN)[None, :] < doc_lens[:, None]).astype(jnp.int32)
    base_state = 0.6 * shared + 0.6 * topic_vec
    query_hidden = base_state + concept
    doc_concept = jnp.take(concept, jnp.arange(DLEN) % QLEN, axis=1)
    real_tok = base_state + 0.6 * doc_concept + 0.8 * token_noise
    pad_tok = 1.5 * shared + token_noise
    doc_hidden = jnp.where(doc_mask[:, :, None] > 0, real_tok, pad_tok)
    w_proj = jax.random.normal(key_weight, (HIDDEN, PROJ), jnp.float32) * HIDDEN ** -0.5
    temperature = QLEN * jax.random.uniform(key_temp, (), jnp.float32, 0.8, 1.25) / 8.0
    return {'query_hidden': query_hidden.astype(jnp.bfloat16), 'doc_hidden': doc_hidden.astype(jnp.bfloat16), 'w_proj': w_proj.astype(jnp.bfloat16), 'query_mask': query_mask, 'doc_mask': doc_mask, 'temperature': temperature}


def project_norm(hidden, w_proj):
    flat_states = hidden.reshape(-1, HIDDEN)
    projected = jnp.dot(flat_states, w_proj, preferred_element_type=jnp.float32)
    norm_len = jnp.sqrt(jnp.sum(projected * projected, axis=-1, keepdims=True))
    unit_vecs = projected / jnp.maximum(norm_len, 1e-12)
    return unit_vecs.astype(jnp.bfloat16).reshape(hidden.shape[0], hidden.shape[1], PROJ)


def reference(query_hidden, doc_hidden, w_proj, query_mask, doc_mask, temperature):
    q_vecs = project_norm(query_hidden, w_proj)
    p_vecs = project_norm(doc_hidden, w_proj).astype(jnp.float32)
    doc_valid = doc_mask[None, :, :] > 0

    def query_row(query_args):
        q_tok, q_weight = query_args
        similarity = jnp.einsum('tc,jsc->tjs', q_tok.astype(jnp.float32), p_vecs)
        best_match = jnp.max(jnp.where(doc_valid, similarity, -jnp.inf), axis=-1)
        return jnp.sum(q_weight.astype(jnp.float32)[:, None] * best_match, axis=0)

    scores = lax.map(query_row, (q_vecs, query_mask))
    logits = scores / temperature
    losses = jax.nn.logsumexp(logits, axis=1) - jnp.diagonal(logits)
    mean_loss = jnp.mean(losses).reshape(1)
    return losses, mean_loss
```

```python
import functools

import jax
import jax.numpy as jnp
from jax import lax
from jax.experimental import pallas as pl
from jax.experimental.pallas import tpu as pltpu
from jax.sharding import PartitionSpec as P

MESH = pl.DeviceIdType.MESH
F32, BF16 = jnp.float32, jnp.bfloat16
BIG = 1e30
UNIT = 64
LANES = 8
RING = 6


def iota(shape, dim):
    return lax.broadcasted_iota(jnp.int32, shape, dim)


def dot(a, b):
    return jnp.dot(a, b, preferred_element_type=F32)


def place(rel):
    y, d = lax.axis_index('data2'), lax.axis_index('data')
    x, core = d // 2, d % 2
    y = 1 - y if rel & 4 else y
    x = 1 - x if rel & 2 else x
    core = 1 - core if rel & 1 else core
    return {'data2': y, 'data': x * 2 + core}, y * 4 + x * 2 + core


def unit_rows(projected):
    square = jnp.sum(projected * projected, axis=-1, keepdims=True)
    return (projected * lax.rsqrt(jnp.maximum(square, 1e-24))).astype(BF16)


def project_kernel(nq, qlen, nd, dlen, q_hbm, d_hbm, w_hbm, qm_hbm, dm_hbm, q_all, qm_all, p_ext, table,
                   q_buf, w_buf, dm_buf, nmt, d_buf, in_sem, d_sem, qs_sem, qr_sem, ms_sem, mr_sem):
    rows = nq * qlen
    me = place(0)[1]
    my_mask = qm_all.at[pl.ds(me * nq, nq)]
    ins = [pltpu.make_async_copy(src, dst, in_sem.at[k]) for k, (src, dst) in enumerate(
        [(qm_hbm, my_mask), (dm_hbm, dm_buf), (w_hbm, w_buf), (q_hbm, q_buf)])]
    for copy in ins:
        copy.start()

    def doc_copy(j, slot):
        return pltpu.make_async_copy(d_hbm.at[pl.ds(j * dlen, dlen)], d_buf.at[slot], d_sem.at[slot])

    for j in range(RING):
        doc_copy(j, j).start()

    barrier = pltpu.get_barrier_semaphore()
    for rel in (1, 2, 4, 6):
        pl.semaphore_signal(barrier, inc=1, device_id=place(rel)[0], device_id_type=MESH)

    ins[0].wait()
    mask = qm_all[pl.ds(me * nq, nq), :].astype(F32).astype(BF16)
    spread = dot(mask, (iota((qlen, rows), 1) % qlen == iota((qlen, rows), 0)).astype(F32).astype(BF16))
    flat = jnp.sum(jnp.where(iota((nq, rows), 1) // qlen == iota((nq, rows), 0), spread, 0.0), axis=0, keepdims=True)
    before = (iota((rows, rows), 0) < iota((rows, rows), 1)).astype(F32).astype(BF16)
    rank = dot(jnp.broadcast_to(flat, (16, rows)).astype(BF16), before)[0:1]
    rank = jnp.where(flat > 0.5, rank, -1.0).astype(jnp.int32)
    pick = (iota((rows, rows), 0) == rank).astype(F32).astype(BF16)

    ins[1].wait()
    dmask = dm_buf[...]
    off = jnp.concatenate([1.0 - dmask.astype(F32), jnp.zeros((128 - nd, dlen), F32)], axis=0)
    nmt[...] = jnp.transpose(off).astype(BF16)
    last = jnp.max(dmask * (iota((nd, dlen), 1) + 1), axis=1, keepdims=True).astype(F32)
    per_doc = dlen // UNIT
    count = jnp.floor((last + (UNIT - 1.0)) * (1.0 / UNIT))
    wide = jnp.broadcast_to(count, (nd, 128))
    upto = dot((iota((nd, nd), 0) >= iota((nd, nd), 1)).astype(F32).astype(BF16), wide.astype(BF16))[:, 0:1]
    total = jnp.max(upto, axis=0, keepdims=True)
    slot_id = jnp.minimum(iota((nd, 256), 1).astype(F32), total - 1.0)
    passed = slot_id >= upto
    unit = slot_id[0:1] + jnp.sum(jnp.where(passed, per_doc - count, 0.0), axis=0, keepdims=True)
    doc = jnp.sum(jnp.where(passed, 1.0, 0.0), axis=0, keepdims=True)
    table[0:1, :] = unit.astype(jnp.int32)
    table[1:2, :] = doc.astype(jnp.int32)
    table[2:3, :] = jnp.broadcast_to(total, (1, 256)).astype(jnp.int32)

    ins[2].wait()
    ins[3].wait()
    q_vec = unit_rows(dot(q_buf[...], w_buf[...]))
    q_all[pl.ds(me * rows, rows), :] = dot(pick, q_vec).astype(BF16)
    pl.semaphore_wait(barrier, 4)

    def send(origin_rel, to_rel, k):
        origin = place(origin_rel)[1]
        arrive = origin_rel ^ to_rel
        target = place(to_rel)[0]
        q_ref, m_ref = q_all.at[pl.ds(origin * rows, rows)], qm_all.at[pl.ds(origin * nq, nq)]
        pair = [pltpu.make_async_remote_copy(src_ref=ref, dst_ref=ref, send_sem=ss.at[k], recv_sem=rs.at[arrive - 1],
                                             device_id=target, device_id_type=MESH)
                for ref, ss, rs in ((m_ref, ms_sem, mr_sem), (q_ref, qs_sem, qr_sem))]
        for copy in pair:
            copy.start()
        return pair

    def received(rel):
        origin = place(rel)[1]
        q_ref, m_ref = q_all.at[pl.ds(origin * rows, rows)], qm_all.at[pl.ds(origin * nq, nq)]
        for ref, ss, rs in ((m_ref, ms_sem, mr_sem), (q_ref, qs_sem, qr_sem)):
            pltpu.make_async_remote_copy(src_ref=ref, dst_ref=ref, send_sem=ss.at[0], recv_sem=rs.at[rel - 1],
                                         device_id=place(rel)[0], device_id_type=MESH).wait_recv()

    sent = [send(0, rel, k) for k, rel in enumerate((2, 4, 6, 1))]

    def project(j, carry):
        slot = lax.rem(j, RING)
        doc_copy(j, slot).wait()
        p_ext[pl.ds(j * dlen, dlen), 0:128] = unit_rows(dot(d_buf[slot], w_buf[...]))
        p_ext[pl.ds(j * dlen, dlen), 128:256] = jnp.where(iota((dlen, 128), 1) == j, nmt[...].astype(F32), 0.0).astype(BF16)

        @pl.when(j + RING < nd)
        def _():
            doc_copy(j + RING, slot).start()

        return carry

    split = (5 * nd) // 8
    lax.fori_loop(0, split, project, 0)
    for k, rel in enumerate((2, 4)):
        received(rel)
        sent.append(send(rel, 1, 4 + k))
    lax.fori_loop(split, nd, project, 0)
    received(6)
    sent.append(send(6, 1, 6))
    for rel in (1, 3, 5, 7):
        received(rel)

    lane = iota((1, 256), 1)
    start = jnp.zeros((1, 1), jnp.int32)
    starts = jnp.zeros((1, 256), jnp.int32)
    for dev in range(8):
        starts = starts + jnp.where(lane == dev, start, 0)
        valid = jnp.sum(jnp.sum(qm_all[dev * nq:(dev + 1) * nq, :].astype(F32), axis=1, keepdims=True), axis=0, keepdims=True)
        start = start + (jnp.floor((valid + 15.0) * (1.0 / 16.0)) * 16.0).astype(jnp.int32)
    table[3:4, :] = starts + jnp.where(lane == 8, start, 0)
    for pair in sent:
        for copy in pair:
            copy.wait_send()


def score_body(nd, rows, tiles, table, q_all, p_ext, out, q_list, best, accs):
    floor = jnp.full((nd, 8, 256), -3e38, F32)
    out[...] = jnp.zeros_like(out)
    for dev in range(8):
        q_list[pl.ds(pl.multiple_of(table[3, dev], 16), rows), :] = q_all[dev * rows:(dev + 1) * rows, :]
    q_list[pl.ds(pl.multiple_of(table[3, 7], 16) + rows, 256), :] = jnp.zeros((256, 128), BF16)
    n_tile = (table[3, 8] + 255) // 256
    n_trip = (table[2, 0] + (2 * LANES - 1)) // (2 * LANES)
    away = jnp.full((256, 128), -BIG, BF16)

    def push(tile):
        q_tile = q_list[pl.ds(pl.multiple_of(tile * 256, 256), 256), :]
        rhs = jnp.concatenate([q_tile, away], axis=1)
        for unit in range(2):
            pltpu.matmul_push_rhs(rhs, staging_register=0, mxu_index=unit, transpose=True)

    def drain(unit, k, slot, trip):
        value = pltpu.matmul_pop(accs[unit][k])
        top = value[0:8]
        for r in range(1, UNIT // 8):
            top = jnp.maximum(top, value[8 * r:8 * r + 8])
        doc = table[1, trip * (2 * LANES) + 2 * k + unit]
        best[unit][slot, doc] = jnp.maximum(best[unit][slot, doc], top)

    def step(slot, trip, prev_slot, prev_trip, first):
        for k in range(LANES):
            for unit in range(2):
                drain(unit, k, prev_slot, prev_trip)
                row = table[0, trip * (2 * LANES) + 2 * k + unit] * UNIT
                lhs = p_ext[pl.ds(pl.multiple_of(row, UNIT), UNIT), :]
                pltpu.matmul_acc_lhs(accs[unit][k], lhs, load_staged_rhs=0 if first and k == 0 else None)

    def finish(slot, tile):
        both = jnp.maximum(best[0][slot], best[1][slot])
        out[tile] = jnp.max(both, axis=1)

    for unit in range(2):
        for k in range(LANES):
            pltpu.matmul_pop(accs[unit][k])
    push(0)

    def per_tile(tile, carry):
        best[0][tile + 1] = floor
        best[1][tile + 1] = floor
        step(tile + 1, 0, tile, n_trip - 1, True)
        finish(tile, jnp.maximum(tile - 1, 0))
        push(jnp.minimum(tile + 1, tiles - 1))

        def per_trip(trip, carry):
            step(tile + 1, trip, tile + 1, trip - 1, False)
            return carry

        lax.fori_loop(1, n_trip, per_trip, 0)
        return carry

    best[0][0] = floor
    best[1][0] = floor
    lax.fori_loop(0, n_tile, per_tile, 0)
    for k in range(LANES):
        for unit in range(2):
            drain(unit, k, n_tile, n_trip - 1)
    finish(n_tile, n_tile - 1)
    for unit in range(2):
        pltpu.matmul_acc_lhs(accs[unit][0], jnp.zeros((UNIT, 256), BF16), load_staged_rhs=0)
        pltpu.matmul_pop(accs[unit][0])


def score_kernel(nd, rows, tiles, table, q_all, p_ext, out, q_list, best0, best1):
    def body(*accs):
        score_body(nd, rows, tiles, table, q_all, p_ext, out, q_list, (best0, best1), (accs[:LANES], accs[LANES:]))

    pl.run_scoped(body, *[pltpu.ACC(0)((UNIT, 256), F32)] * LANES, *[pltpu.ACC(1)((UNIT, 256), F32)] * LANES)


def loss_kernel(nq, nd, qlen, tiles, temp, best, qm_all, losses, mean, seg, scores, send_sem, recv_sem):
    n = nq * 8
    me = place(0)[1]
    barrier = pltpu.get_barrier_semaphore()
    for rel in range(1, 8):
        pl.semaphore_signal(barrier, inc=1, device_id=place(rel)[0], device_id_type=MESH)

    col = iota((n, n), 1)
    row = iota((n, n), 0)
    as_bf = lambda cond: cond.astype(F32).astype(BF16)
    mask = qm_all[...].astype(F32).astype(BF16)
    counts = lax.dot_general(jnp.ones((16, qlen), BF16), mask, (((1,), (1,)), ((), ())), preferred_element_type=F32)
    counts_bf = counts.astype(BF16)
    in_dev = dot(counts_bf, as_bf((row // nq == col // nq) & (row < col)))
    valid = dot(counts_bf, as_bf(row // nq == col // nq))
    padded = jnp.floor((valid + 15.0) * (1.0 / 16.0)) * 16.0
    begin = dot(padded.astype(BF16), as_bf((row // nq < col // nq) & (row % nq == 0))) + in_dev
    first = begin[0:1].astype(jnp.int32)
    end = (begin + counts)[0:1].astype(jnp.int32)
    where = iota((tiles * 256, n), 0)
    seg[...] = as_bf((where >= first) & (where < end))

    total = jnp.zeros((nd, n), F32)
    for t in range(tiles):
        value = best[t]
        high = value.astype(BF16)
        rest = value - high.astype(F32)
        mid = rest.astype(BF16)
        low = (rest - mid.astype(F32)).astype(BF16)
        part = dot(jnp.concatenate([high, mid, low], axis=0), seg[t * 256:(t + 1) * 256, :])
        total = total + ((part[0:nd] + part[nd:2 * nd]) + part[2 * nd:3 * nd])
    mine = scores.at[pl.ds(me * nd, nd)]
    scores[pl.ds(me * nd, nd), :] = total
    pl.semaphore_wait(barrier, 7)
    copies = [pltpu.make_async_remote_copy(src_ref=mine, dst_ref=mine, send_sem=send_sem.at[rel - 1],
                                           recv_sem=recv_sem.at[rel - 1], device_id=place(rel)[0], device_id_type=MESH)
              for rel in (6, 7, 2, 3, 4, 5, 1)]
    for copy in copies:
        copy.start()
    for rel in range(1, 8):
        theirs = scores.at[pl.ds(place(rel)[1] * nd, nd)]
        pltpu.make_async_remote_copy(src_ref=theirs, dst_ref=theirs, send_sem=send_sem.at[rel - 1],
                                     recv_sem=recv_sem.at[rel - 1], device_id=place(rel)[0],
                                     device_id_type=MESH).wait_recv()

    logits = scores[...] / temp[0]
    own = jnp.sum(jnp.where(row == col, logits, 0.0), axis=0, keepdims=True)
    peak = jnp.max(logits, axis=0, keepdims=True)
    loss = jnp.log(jnp.sum(jnp.exp(logits - peak), axis=0, keepdims=True)) + peak - own
    mean[...] = jnp.sum(loss, axis=1, keepdims=True) / n
    small_row, small_col = iota((nq, n), 0), iota((nq, n), 1)
    picked = jnp.sum(jnp.where(small_col == me * nq + small_row, loss, 0.0), axis=1, keepdims=True)
    losses[...] = jnp.sum(jnp.where(small_col == small_row, picked, 0.0), axis=0, keepdims=True)[:, 0:nq]
    for copy in copies:
        copy.wait_send()


VMEM = pl.BlockSpec(memory_space=pltpu.VMEM)
SMEM = pl.BlockSpec(memory_space=pltpu.SMEM)
ANY = pl.BlockSpec(memory_space=pl.ANY)
DMA = pltpu.SemaphoreType.DMA


def solution(mesh):
    def local_step(query_hidden, doc_hidden, w_proj, query_mask, doc_mask, temperature):
        nq, qlen, hidden = query_hidden.shape
        nd, dlen, _ = doc_hidden.shape
        rows = nq * qlen
        tiles = rows * 8 // 256
        hbm = lambda x: pltpu.with_memory_space_constraint(x, pltpu.HBM)
        vmem = lambda x: pltpu.with_memory_space_constraint(x, pltpu.VMEM)
        q_all, qm_all, p_ext, table = pl.pallas_call(
            functools.partial(project_kernel, nq, qlen, nd, dlen),
            out_shape=[
                pltpu.VMEM((rows * 8, 128), BF16),
                pltpu.VMEM((nq * 8, qlen), jnp.int32),
                pltpu.VMEM((nd * dlen, 256), BF16),
                pltpu.VMEM((8, 256), jnp.int32),
            ],
            in_specs=[ANY] * 5,
            out_specs=[VMEM] * 4,
            scratch_shapes=[
                pltpu.VMEM((rows, hidden), BF16),
                pltpu.VMEM((hidden, 128), BF16),
                pltpu.VMEM((nd, dlen), jnp.int32),
                pltpu.VMEM((dlen, 128), BF16),
                pltpu.VMEM((RING, dlen, hidden), BF16),
                DMA((4,)), DMA((RING,)), DMA((7,)), DMA((7,)), DMA((7,)), DMA((7,)),
            ],
            compiler_params=pltpu.CompilerParams(collective_id=0, has_side_effects=True, vmem_limit_bytes=50 * 2**20),
            name='project',
        )(hbm(query_hidden.reshape(rows, hidden)), hbm(doc_hidden.reshape(nd * dlen, hidden)), hbm(w_proj),
          hbm(query_mask), hbm(doc_mask))

        best = pl.pallas_call(
            functools.partial(score_kernel, nd, rows, tiles),
            out_shape=pltpu.VMEM((tiles, nd, 256), F32),
            in_specs=[SMEM, VMEM, VMEM],
            out_specs=VMEM,
            scratch_shapes=[
                pltpu.VMEM((rows * 8 + 512, 128), BF16),
                pltpu.VMEM((tiles + 1, nd, 8, 256), F32),
                pltpu.VMEM((tiles + 1, nd, 8, 256), F32),
            ],
            compiler_params=pltpu.CompilerParams(vmem_limit_bytes=30 * 2**20),
            name='score',
        )(table, vmem(q_all), vmem(p_ext))

        losses, mean = pl.pallas_call(
            functools.partial(loss_kernel, nq, nd, qlen, tiles),
            out_shape=[jax.ShapeDtypeStruct((1, nq), F32), jax.ShapeDtypeStruct((1, 1), F32)],
            in_specs=[SMEM, VMEM, VMEM],
            out_specs=[VMEM, VMEM],
            scratch_shapes=[
                pltpu.VMEM((tiles * 256, nq * 8), BF16),
                pltpu.VMEM((nd * 8, nq * 8), F32),
                DMA((7,)), DMA((7,)),
            ],
            compiler_params=pltpu.CompilerParams(collective_id=1, has_side_effects=True),
            name='loss',
        )(temperature.reshape(1), vmem(best), vmem(qm_all))
        return losses.reshape(nq), mean.reshape(1)

    tok, mask, row = P(('replica', 'data2', 'data'), None, None), P(('replica', 'data2', 'data'), None), P(('replica', 'data2', 'data'))
    return jax.shard_map(local_step, mesh=mesh, in_specs=(tok, tok, P(None, None), mask, mask, P()),
                         out_specs=(row, P('replica')), check_vma=False)
```

```python
import functools

import jax
import jax.numpy as jnp
from jax import lax
from jax.experimental import pallas as pl
from jax.experimental.pallas import tpu as pltpu
from jax.sharding import PartitionSpec as P

MESH = pl.DeviceIdType.MESH
F32, BF16 = jnp.float32, jnp.bfloat16
BIG = 1e30
UNIT = 64
LANES = 8
RING = 6


def iota(shape, dim):
    return lax.broadcasted_iota(jnp.int32, shape, dim)


def dot(a, b):
    return jnp.dot(a, b, preferred_element_type=F32)


def place(rel):
    y, d = lax.axis_index('data2'), lax.axis_index('data')
    x, core = d // 2, d % 2
    y = 1 - y if rel & 4 else y
    x = 1 - x if rel & 2 else x
    core = 1 - core if rel & 1 else core
    return {'data2': y, 'data': x * 2 + core}, y * 4 + x * 2 + core


def unit_rows(projected):
    square = jnp.sum(projected * projected, axis=-1, keepdims=True)
    return (projected * lax.rsqrt(jnp.maximum(square, 1e-24))).astype(BF16)


def project_kernel(nq, qlen, nd, dlen, q_hbm, d_hbm, w_hbm, qm_hbm, dm_hbm, q_all, p_ext, table, seg,
                   qm_all, q_buf, w_buf, dm_buf, nmt, d_buf, in_sem, d_sem, qs_sem, qr_sem, ms_sem, mr_sem):
    rows = nq * qlen
    n = nq * 8
    me = place(0)[1]
    as_bf = lambda cond: cond.astype(F32).astype(BF16)
    ins = [pltpu.make_async_copy(src, dst, in_sem.at[k]) for k, (src, dst) in enumerate(
        [(qm_hbm, qm_all.at[pl.ds(me * nq, nq)]), (dm_hbm, dm_buf), (w_hbm, w_buf), (q_hbm, q_buf)])]
    for copy in ins:
        copy.start()

    def doc_copy(j, slot):
        return pltpu.make_async_copy(d_hbm.at[pl.ds(j * dlen, dlen)], d_buf.at[slot], d_sem.at[slot])

    for j in range(RING):
        doc_copy(j, j).start()

    barrier = pltpu.get_barrier_semaphore()
    for rel in range(1, 8):
        pl.semaphore_signal(barrier, inc=1, device_id=place(rel)[0], device_id_type=MESH)

    def remote(ref, per, origin_rel, to_rel, send_sem, recv_sem):
        block = ref.at[pl.ds(place(origin_rel)[1] * per, per)]
        return pltpu.make_async_remote_copy(src_ref=block, dst_ref=block, send_sem=send_sem, recv_sem=recv_sem,
                                            device_id=place(to_rel)[0], device_id_type=MESH)

    ins[0].wait()
    pl.semaphore_wait(barrier, 7)
    mask_sent = [remote(qm_all, nq, 0, rel, ms_sem.at[rel - 1], mr_sem.at[rel - 1]) for rel in (6, 7, 2, 3, 4, 5, 1)]
    for copy in mask_sent:
        copy.start()

    mask = qm_all[pl.ds(me * nq, nq), :].astype(F32).astype(BF16)
    spread = dot(mask, as_bf(iota((qlen, rows), 1) % qlen == iota((qlen, rows), 0)))
    flat = jnp.sum(jnp.where(iota((nq, rows), 1) // qlen == iota((nq, rows), 0), spread, 0.0), axis=0, keepdims=True)
    before = as_bf(iota((rows, rows), 0) < iota((rows, rows), 1))
    rank = dot(jnp.broadcast_to(flat, (16, rows)).astype(BF16), before)[0:1]
    rank = jnp.where(flat > 0.5, rank, -1.0).astype(jnp.int32)
    pick = as_bf(iota((rows, rows), 0) == rank)

    ins[2].wait()
    ins[3].wait()
    q_vec = unit_rows(dot(q_buf[...], w_buf[...]))
    q_all[pl.ds(me * rows, rows), :] = dot(pick, q_vec).astype(BF16)
    sent = []

    def send(origin_rel, to_rel):
        copy = remote(q_all, rows, origin_rel, to_rel, qs_sem.at[len(sent)], qr_sem.at[(origin_rel ^ to_rel) - 1])
        copy.start()
        sent.append(copy)

    def received(rel):
        remote(q_all, rows, rel, rel, qs_sem.at[0], qr_sem.at[rel - 1]).wait_recv()

    for rel in (2, 4, 6, 1):
        send(0, rel)

    ins[1].wait()
    dmask = dm_buf[...]
    off = jnp.concatenate([1.0 - dmask.astype(F32), jnp.zeros((128 - nd, dlen), F32)], axis=0)
    nmt[...] = jnp.transpose(off).astype(BF16)
    last = jnp.max(dmask * (iota((nd, dlen), 1) + 1), axis=1, keepdims=True).astype(F32)
    per_doc = dlen // UNIT
    count = jnp.floor((last + (UNIT - 1.0)) * (1.0 / UNIT))
    wide = jnp.broadcast_to(count, (nd, 128))
    upto = dot(as_bf(iota((nd, nd), 0) >= iota((nd, nd), 1)), wide.astype(BF16))[:, 0:1]
    total = jnp.max(upto, axis=0, keepdims=True)
    slot_id = jnp.minimum(iota((nd, 256), 1).astype(F32), total - 1.0)
    passed = slot_id >= upto
    unit = slot_id[0:1] + jnp.sum(jnp.where(passed, per_doc - count, 0.0), axis=0, keepdims=True)
    doc = jnp.sum(jnp.where(passed, 1.0, 0.0), axis=0, keepdims=True)
    table[0:1, :] = unit.astype(jnp.int32)
    table[1:2, :] = doc.astype(jnp.int32)
    table[2:3, :] = jnp.broadcast_to(total, (1, 256)).astype(jnp.int32)

    def project(j, carry):
        slot = lax.rem(j, RING)
        doc_copy(j, slot).wait()
        p_ext[pl.ds(j * dlen, dlen), 0:128] = unit_rows(dot(d_buf[slot], w_buf[...]))
        p_ext[pl.ds(j * dlen, dlen), 128:256] = jnp.where(iota((dlen, 128), 1) == j, nmt[...].astype(F32), 0.0).astype(BF16)

        @pl.when(j + RING < nd)
        def _():
            doc_copy(j + RING, slot).start()

        return carry

    cut1, cut2 = (7 * nd) // 16, (12 * nd) // 16
    lax.fori_loop(0, cut1, project, 0)
    for rel in (2, 4):
        received(rel)
        send(rel, 1)

    for rel in range(1, 8):
        remote(qm_all, nq, rel, rel, ms_sem.at[rel - 1], mr_sem.at[rel - 1]).wait_recv()
    row, col = iota((n, n), 0), iota((n, n), 1)
    every = qm_all[...].astype(F32).astype(BF16)
    counts = lax.dot_general(jnp.ones((16, qlen), BF16), every, (((1,), (1,)), ((), ())), preferred_element_type=F32)
    counts_bf = counts.astype(BF16)
    in_dev = dot(counts_bf, as_bf((row // nq == col // nq) & (row < col)))
    padded = jnp.floor((dot(counts_bf, as_bf(row // nq == col // nq)) + 15.0) * (1.0 / 16.0)) * 16.0
    padded_bf = padded.astype(BF16)
    begin = dot(padded_bf, as_bf((row // nq < col // nq) & (row % nq == 0))) + in_dev
    starts = dot(padded_bf, as_bf((row // nq < col) & (row % nq == 0)))
    table[3:4, 0:128] = starts[0:1].astype(jnp.int32)
    table[3:4, 128:256] = starts[0:1].astype(jnp.int32)
    first = begin[0:1].astype(jnp.int32)
    end = (begin + counts)[0:1].astype(jnp.int32)
    where = iota((rows * 8, n), 0)
    seg[...] = as_bf((where >= first) & (where < end))

    lax.fori_loop(cut1, cut2, project, 0)
    received(6)
    send(6, 1)
    lax.fori_loop(cut2, nd, project, 0)
    for rel in (1, 3, 5, 7):
        received(rel)
    for copy in mask_sent + sent:
        copy.wait_send()


def score_body(nd, rows, tiles, table, q_all, p_ext, out, q_list, best, accs):
    floor = jnp.full((nd, 8, 256), -3e38, F32)
    out[...] = jnp.zeros_like(out)
    for dev in range(8):
        q_list[pl.ds(pl.multiple_of(table[3, dev], 16), rows), :] = q_all[dev * rows:(dev + 1) * rows, :]
    q_list[pl.ds(pl.multiple_of(table[3, 7], 16) + rows, 256), :] = jnp.zeros((256, 128), BF16)
    n_tile = (table[3, 8] + 255) // 256
    n_trip = (table[2, 0] + (2 * LANES - 1)) // (2 * LANES)
    away = jnp.full((256, 128), -BIG, BF16)

    def push(tile):
        q_tile = q_list[pl.ds(pl.multiple_of(tile * 256, 256), 256), :]
        rhs = jnp.concatenate([q_tile, away], axis=1)
        for unit in range(2):
            pltpu.matmul_push_rhs(rhs, staging_register=0, mxu_index=unit, transpose=True)

    def drain(unit, k, slot, trip):
        value = pltpu.matmul_pop(accs[unit][k])
        top = value[0:8]
        for r in range(1, UNIT // 8):
            top = jnp.maximum(top, value[8 * r:8 * r + 8])
        doc = table[1, trip * (2 * LANES) + 2 * k + unit]
        best[unit][slot, doc] = jnp.maximum(best[unit][slot, doc], top)

    def step(slot, trip, prev_slot, prev_trip, first):
        for k in range(LANES):
            for unit in range(2):
                drain(unit, k, prev_slot, prev_trip)
                row = table[0, trip * (2 * LANES) + 2 * k + unit] * UNIT
                lhs = p_ext[pl.ds(pl.multiple_of(row, UNIT), UNIT), :]
                pltpu.matmul_acc_lhs(accs[unit][k], lhs, load_staged_rhs=0 if first and k == 0 else None)

    def finish(slot, tile):
        both = jnp.maximum(best[0][slot], best[1][slot])
        out[tile] = jnp.max(both, axis=1)

    for unit in range(2):
        for k in range(LANES):
            pltpu.matmul_pop(accs[unit][k])
    push(0)

    def per_tile(tile, carry):
        best[0][tile + 1] = floor
        best[1][tile + 1] = floor
        step(tile + 1, 0, tile, n_trip - 1, True)
        finish(tile, jnp.maximum(tile - 1, 0))
        push(jnp.minimum(tile + 1, tiles - 1))

        def per_trip(trip, carry):
            step(tile + 1, trip, tile + 1, trip - 1, False)
            return carry

        lax.fori_loop(1, n_trip, per_trip, 0)
        return carry

    best[0][0] = floor
    best[1][0] = floor
    lax.fori_loop(0, n_tile, per_tile, 0)
    for k in range(LANES):
        for unit in range(2):
            drain(unit, k, n_tile, n_trip - 1)
    finish(n_tile, n_tile - 1)
    for unit in range(2):
        pltpu.matmul_acc_lhs(accs[unit][0], jnp.zeros((UNIT, 256), BF16), load_staged_rhs=0)
        pltpu.matmul_pop(accs[unit][0])


def score_kernel(nd, rows, tiles, table, q_all, p_ext, out, q_list, best0, best1):
    def body(*accs):
        score_body(nd, rows, tiles, table, q_all, p_ext, out, q_list, (best0, best1), (accs[:LANES], accs[LANES:]))

    pl.run_scoped(body, *[pltpu.ACC(0)((UNIT, 256), F32)] * LANES, *[pltpu.ACC(1)((UNIT, 256), F32)] * LANES)


def gather_kernel(nd, tiles, temp, best, seg, scores, send_sem, recv_sem):
    me = place(0)[1]
    barrier = pltpu.get_barrier_semaphore()
    for rel in range(1, 8):
        pl.semaphore_signal(barrier, inc=1, device_id=place(rel)[0], device_id_type=MESH)
    total = jnp.zeros((nd, nd * 8), F32)
    for t in range(tiles):
        value = best[t]
        high = value.astype(BF16)
        rest = value - high.astype(F32)
        mid = rest.astype(BF16)
        low = (rest - mid.astype(F32)).astype(BF16)
        part = dot(jnp.concatenate([high, mid, low], axis=0), seg[t * 256:(t + 1) * 256, :])
        total = total + ((part[0:nd] + part[nd:2 * nd]) + part[2 * nd:3 * nd])
    scores[pl.ds(me * nd, nd), :] = total / temp[0]
    pl.semaphore_wait(barrier, 7)

    def remote(origin_rel, rel):
        block = scores.at[pl.ds(place(origin_rel)[1] * nd, nd)]
        return pltpu.make_async_remote_copy(src_ref=block, dst_ref=block, send_sem=send_sem.at[rel - 1],
                                            recv_sem=recv_sem.at[rel - 1], device_id=place(rel)[0], device_id_type=MESH)

    copies = [remote(0, rel) for rel in (6, 7, 2, 3, 4, 5, 1)]
    for copy in copies:
        copy.start()
    for rel in range(1, 8):
        remote(rel, rel).wait_recv()
    for copy in copies:
        copy.wait_send()


def loss_kernel(nq, scores, losses, mean):
    n = nq * 8
    me = place(0)[1]
    logits = scores[...]
    own = jnp.sum(jnp.where(iota((n, n), 0) == iota((n, n), 1), logits, 0.0), axis=0, keepdims=True)
    peak = jnp.max(logits, axis=0, keepdims=True)
    loss = jnp.log(jnp.sum(jnp.exp(logits - peak), axis=0, keepdims=True)) + peak - own
    mean[...] = jnp.sum(loss, axis=1, keepdims=True) / n
    row, col = iota((nq, n), 0), iota((nq, n), 1)
    picked = jnp.sum(jnp.where(col == me * nq + row, loss, 0.0), axis=1, keepdims=True)
    losses[...] = jnp.sum(jnp.where(col == row, picked, 0.0), axis=0, keepdims=True)[:, 0:nq]


VMEM = pl.BlockSpec(memory_space=pltpu.VMEM)
SMEM = pl.BlockSpec(memory_space=pltpu.SMEM)
ANY = pl.BlockSpec(memory_space=pl.ANY)
DMA = pltpu.SemaphoreType.DMA


def solution(mesh):
    def local_step(query_hidden, doc_hidden, w_proj, query_mask, doc_mask, temperature):
        nq, qlen, hidden = query_hidden.shape
        nd, dlen, _ = doc_hidden.shape
        rows = nq * qlen
        tiles = rows * 8 // 256
        hbm = lambda x: pltpu.with_memory_space_constraint(x, pltpu.HBM)
        vmem = lambda x: pltpu.with_memory_space_constraint(x, pltpu.VMEM)
        q_all, p_ext, table, seg = pl.pallas_call(
            functools.partial(project_kernel, nq, qlen, nd, dlen),
            out_shape=[
                pltpu.VMEM((rows * 8, 128), BF16),
                pltpu.VMEM((nd * dlen, 256), BF16),
                pltpu.VMEM((8, 256), jnp.int32),
                pltpu.VMEM((rows * 8, nq * 8), BF16),
            ],
            in_specs=[ANY] * 5,
            out_specs=[VMEM] * 4,
            scratch_shapes=[
                pltpu.VMEM((nq * 8, qlen), jnp.int32),
                pltpu.VMEM((rows, hidden), BF16),
                pltpu.VMEM((hidden, 128), BF16),
                pltpu.VMEM((nd, dlen), jnp.int32),
                pltpu.VMEM((dlen, 128), BF16),
                pltpu.VMEM((RING, dlen, hidden), BF16),
                DMA((4,)), DMA((RING,)), DMA((7,)), DMA((7,)), DMA((7,)), DMA((7,)),
            ],
            compiler_params=pltpu.CompilerParams(collective_id=0, has_side_effects=True, vmem_limit_bytes=50 * 2**20),
            name='project',
        )(hbm(query_hidden.reshape(rows, hidden)), hbm(doc_hidden.reshape(nd * dlen, hidden)), hbm(w_proj),
          hbm(query_mask), hbm(doc_mask))

        best = pl.pallas_call(
            functools.partial(score_kernel, nd, rows, tiles),
            out_shape=pltpu.VMEM((tiles, nd, 256), F32),
            in_specs=[SMEM, VMEM, VMEM],
            out_specs=VMEM,
            scratch_shapes=[
                pltpu.VMEM((rows * 8 + 512, 128), BF16),
                pltpu.VMEM((tiles + 1, nd, 8, 256), F32),
                pltpu.VMEM((tiles + 1, nd, 8, 256), F32),
            ],
            compiler_params=pltpu.CompilerParams(vmem_limit_bytes=30 * 2**20),
            name='score',
        )(table, vmem(q_all), vmem(p_ext))

        scores = pl.pallas_call(
            functools.partial(gather_kernel, nd, tiles),
            out_shape=pltpu.VMEM((nd * 8, nq * 8), F32),
            in_specs=[SMEM, VMEM, VMEM],
            out_specs=VMEM,
            scratch_shapes=[DMA((7,)), DMA((7,))],
            compiler_params=pltpu.CompilerParams(collective_id=1, has_side_effects=True),
            name='gather',
        )(temperature.reshape(1), vmem(best), vmem(seg))

        losses, mean = pl.pallas_call(
            functools.partial(loss_kernel, nq),
            out_shape=[jax.ShapeDtypeStruct((1, nq), F32), jax.ShapeDtypeStruct((1, 1), F32)],
            in_specs=[VMEM],
            out_specs=[VMEM, VMEM],
            name='loss',
        )(vmem(scores))
        return losses.reshape(nq), mean.reshape(1)

    tok, mask, row = P(('replica', 'data2', 'data'), None, None), P(('replica', 'data2', 'data'), None), P(('replica', 'data2', 'data'))
    return jax.shard_map(local_step, mesh=mesh, in_specs=(tok, tok, P(None, None), mask, mask, P()),
                         out_specs=(row, P('replica')), check_vma=False)
```

```python
import functools

import jax
import jax.numpy as jnp
from jax import lax
from jax.experimental import pallas as pl
from jax.experimental.pallas import tpu as pltpu
from jax.sharding import PartitionSpec as P

MESH = pl.DeviceIdType.MESH
F32, BF16 = jnp.float32, jnp.bfloat16
BIG = 1e30
UNIT = 64
LANES = 8
RING = 4
HEAD = 256
GROUP = 4
TAIL_RING = 8


def iota(shape, dim):
    return lax.broadcasted_iota(jnp.int32, shape, dim)


def dot(a, b):
    return jnp.dot(a, b, preferred_element_type=F32)


def place(rel):
    y, d = lax.axis_index('data2'), lax.axis_index('data')
    x, core = d // 2, d % 2
    y = 1 - y if rel & 4 else y
    x = 1 - x if rel & 2 else x
    core = 1 - core if rel & 1 else core
    return {'data2': y, 'data': x * 2 + core}, y * 4 + x * 2 + core


def unit_rows(projected):
    square = jnp.sum(projected * projected, axis=-1, keepdims=True)
    return (projected * lax.rsqrt(jnp.maximum(square, 1e-24))).astype(BF16)


def mask_features(doc, off):
    return jnp.where(iota(off.shape, 1) == doc, off.astype(F32), 0.0).astype(BF16)


def project_kernel(nq, qlen, nd, dlen, q_hbm, d_hbm, w_hbm, qm_hbm, dm_hbm, q_all, p_ext, table, seg, nmt,
                   qm_all, q_buf, w_buf, dm_buf, d_buf, in_sem, d_sem, qs_sem, qr_sem, ms_sem, mr_sem):
    rows = nq * qlen
    n = nq * 8
    me = place(0)[1]
    as_bf = lambda cond: cond.astype(F32).astype(BF16)
    ins = [pltpu.make_async_copy(src, dst, in_sem.at[k]) for k, (src, dst) in enumerate(
        [(qm_hbm, qm_all.at[pl.ds(me * nq, nq)]), (dm_hbm, dm_buf), (w_hbm, w_buf), (q_hbm, q_buf)])]
    for copy in ins:
        copy.start()

    def doc_copy(j, slot):
        return pltpu.make_async_copy(d_hbm.at[pl.ds(j * dlen, HEAD)], d_buf.at[slot], d_sem.at[slot])

    for j in range(RING):
        doc_copy(j, j).start()

    barrier = pltpu.get_barrier_semaphore()
    for rel in range(1, 8):
        pl.semaphore_signal(barrier, inc=1, device_id=place(rel)[0], device_id_type=MESH)

    def remote(ref, per, origin_rel, to_rel, send_sem, recv_sem):
        block = ref.at[pl.ds(place(origin_rel)[1] * per, per)]
        return pltpu.make_async_remote_copy(src_ref=block, dst_ref=block, send_sem=send_sem, recv_sem=recv_sem,
                                            device_id=place(to_rel)[0], device_id_type=MESH)

    ins[0].wait()
    pl.semaphore_wait(barrier, 7)
    mask_sent = [remote(qm_all, nq, 0, rel, ms_sem.at[rel - 1], mr_sem.at[rel - 1]) for rel in (6, 7, 2, 3, 4, 5, 1)]
    for copy in mask_sent:
        copy.start()

    mask = qm_all[pl.ds(me * nq, nq), :].astype(F32).astype(BF16)
    spread = dot(mask, as_bf(iota((qlen, rows), 1) % qlen == iota((qlen, rows), 0)))
    flat = jnp.sum(jnp.where(iota((nq, rows), 1) // qlen == iota((nq, rows), 0), spread, 0.0), axis=0, keepdims=True)
    before = as_bf(iota((rows, rows), 0) < iota((rows, rows), 1))
    rank = dot(jnp.broadcast_to(flat, (16, rows)).astype(BF16), before)[0:1]
    rank = jnp.where(flat > 0.5, rank, -1.0).astype(jnp.int32)
    pick = as_bf(iota((rows, rows), 0) == rank)

    ins[2].wait()
    ins[3].wait()
    q_vec = unit_rows(dot(q_buf[...], w_buf[...]))
    q_all[pl.ds(me * rows, rows), :] = dot(pick, q_vec).astype(BF16)
    sent = []

    def send(origin_rel, to_rel):
        copy = remote(q_all, rows, origin_rel, to_rel, qs_sem.at[len(sent)], qr_sem.at[(origin_rel ^ to_rel) - 1])
        copy.start()
        sent.append(copy)

    def received(rel):
        remote(q_all, rows, rel, rel, qs_sem.at[0], qr_sem.at[rel - 1]).wait_recv()

    for rel in (2, 4, 6, 1):
        send(0, rel)

    ins[1].wait()
    dmask = dm_buf[...]
    off = jnp.concatenate([1.0 - dmask.astype(F32), jnp.zeros((128 - nd, dlen), F32)], axis=0)
    nmt[...] = jnp.transpose(off).astype(BF16)
    last = jnp.max(dmask * (iota((nd, dlen), 1) + 1), axis=1, keepdims=True).astype(F32)
    per_doc = dlen // UNIT
    count = jnp.floor((last + (UNIT - 1.0)) * (1.0 / UNIT))
    sums = as_bf(iota((nd, nd), 0) >= iota((nd, nd), 1))

    def listing(at, count, first):
        upto = dot(sums, jnp.broadcast_to(count, (nd, 128)).astype(BF16))[:, 0:1]
        total = jnp.max(upto, axis=0, keepdims=True)
        slot_id = jnp.minimum(iota((nd, 256), 1).astype(F32), jnp.maximum(total - 1.0, 0.0))
        passed = slot_id >= upto
        unit = slot_id[0:1] + first + jnp.sum(jnp.where(passed, per_doc - count, 0.0), axis=0, keepdims=True)
        doc = jnp.sum(jnp.where(passed, 1.0, 0.0), axis=0, keepdims=True)
        table[at:at + 1, :] = unit.astype(jnp.int32)
        table[at + 1:at + 2, :] = doc.astype(jnp.int32)
        table[at + 2:at + 3, :] = jnp.broadcast_to(total, (1, 256)).astype(jnp.int32)

    listing(0, count, 0.0)
    listing(4, jnp.maximum(count - HEAD // UNIT, 0.0), float(HEAD // UNIT))

    def project(j, carry):
        slot = lax.rem(j, RING)
        doc_copy(j, slot).wait()
        p_ext[pl.ds(j * dlen, HEAD), 0:128] = unit_rows(dot(d_buf[slot], w_buf[...]))
        p_ext[pl.ds(j * dlen, HEAD), 128:256] = mask_features(j, nmt[0:HEAD, :])

        @pl.when(j + RING < nd)
        def _():
            doc_copy(j + RING, slot).start()

        return carry

    lax.fori_loop(0, nd, project, 0)
    for rel in (2, 4):
        received(rel)
        send(rel, 1)

    for rel in range(1, 8):
        remote(qm_all, nq, rel, rel, ms_sem.at[rel - 1], mr_sem.at[rel - 1]).wait_recv()
    row, col = iota((n, n), 0), iota((n, n), 1)
    every = qm_all[...].astype(F32).astype(BF16)
    counts = lax.dot_general(jnp.ones((16, qlen), BF16), every, (((1,), (1,)), ((), ())), preferred_element_type=F32)
    counts_bf = counts.astype(BF16)
    in_dev = dot(counts_bf, as_bf((row // nq == col // nq) & (row < col)))
    padded = jnp.floor((dot(counts_bf, as_bf(row // nq == col // nq)) + 15.0) * (1.0 / 16.0)) * 16.0
    padded_bf = padded.astype(BF16)
    begin = dot(padded_bf, as_bf((row // nq < col // nq) & (row % nq == 0))) + in_dev
    starts = dot(padded_bf, as_bf((row // nq < col) & (row % nq == 0)))
    table[3:4, 0:128] = starts[0:1].astype(jnp.int32)
    table[3:4, 128:256] = starts[0:1].astype(jnp.int32)
    first = begin[0:1].astype(jnp.int32)
    end = (begin + counts)[0:1].astype(jnp.int32)
    where = iota((rows * 8, n), 0)
    seg[...] = as_bf((where >= first) & (where < end))

    received(6)
    send(6, 1)
    for rel in (1, 3, 5, 7):
        received(rel)
    for copy in mask_sent + sent:
        copy.wait_send()


def tail_kernel(per_doc, table, d_hbm, w, nmt, p_head, p_ext, d_buf, sem):
    steps = (table[6, 0] + (GROUP - 1)) // GROUP

    def copies(g):
        slot = lax.rem(g, TAIL_RING)
        return [pltpu.make_async_copy(d_hbm.at[pl.ds(pl.multiple_of(table[4, g * GROUP + k] * UNIT, UNIT), UNIT)],
                                      d_buf.at[slot, pl.ds(k * UNIT, UNIT)], sem.at[slot]) for k in range(GROUP)]

    for g in range(TAIL_RING):
        @pl.when(g < steps)
        def _():
            for copy in copies(g):
                copy.start()

    def step(g, carry):
        for copy in copies(g):
            copy.wait()
        value = unit_rows(dot(d_buf[lax.rem(g, TAIL_RING)], w[...]))
        for k in range(GROUP):
            unit, doc = table[4, g * GROUP + k], table[5, g * GROUP + k]
            at = pl.ds(pl.multiple_of(unit * UNIT, UNIT), UNIT)
            p_ext[at, 0:128] = value[k * UNIT:(k + 1) * UNIT]
            p_ext[at, 128:256] = mask_features(doc, nmt[pl.ds(pl.multiple_of((unit - doc * per_doc) * UNIT, UNIT), UNIT), :])

        @pl.when(g + TAIL_RING < steps)
        def _():
            for copy in copies(g + TAIL_RING):
                copy.start()

        return carry

    lax.fori_loop(0, steps, step, 0)


def score_body(nd, rows, tiles, table, q_all, p_ext, out, q_list, best, accs):
    floor = jnp.full((nd, 8, 256), -3e38, F32)
    out[...] = jnp.zeros_like(out)
    for dev in range(8):
        q_list[pl.ds(pl.multiple_of(table[3, dev], 16), rows), :] = q_all[dev * rows:(dev + 1) * rows, :]
    q_list[pl.ds(pl.multiple_of(table[3, 7], 16) + rows, 256), :] = jnp.zeros((256, 128), BF16)
    n_tile = (table[3, 8] + 255) // 256
    n_trip = (table[2, 0] + (2 * LANES - 1)) // (2 * LANES)
    away = jnp.full((256, 128), -BIG, BF16)

    def push(tile):
        q_tile = q_list[pl.ds(pl.multiple_of(tile * 256, 256), 256), :]
        rhs = jnp.concatenate([q_tile, away], axis=1)
        for unit in range(2):
            pltpu.matmul_push_rhs(rhs, staging_register=0, mxu_index=unit, transpose=True)

    def drain(unit, k, slot, trip):
        value = pltpu.matmul_pop(accs[unit][k])
        top = value[0:8]
        for r in range(1, UNIT // 8):
            top = jnp.maximum(top, value[8 * r:8 * r + 8])
        doc = table[1, trip * (2 * LANES) + 2 * k + unit]
        best[unit][slot, doc] = jnp.maximum(best[unit][slot, doc], top)

    def step(slot, trip, prev_slot, prev_trip, first):
        for k in range(LANES):
            for unit in range(2):
                drain(unit, k, prev_slot, prev_trip)
                row = table[0, trip * (2 * LANES) + 2 * k + unit] * UNIT
                lhs = p_ext[pl.ds(pl.multiple_of(row, UNIT), UNIT), :]
                pltpu.matmul_acc_lhs(accs[unit][k], lhs, load_staged_rhs=0 if first and k == 0 else None)

    def finish(slot, tile):
        both = jnp.maximum(best[0][slot], best[1][slot])
        out[tile] = jnp.max(both, axis=1)

    for unit in range(2):
        for k in range(LANES):
            pltpu.matmul_pop(accs[unit][k])
    push(0)

    def per_tile(tile, carry):
        best[0][tile + 1] = floor
        best[1][tile + 1] = floor
        step(tile + 1, 0, tile, n_trip - 1, True)
        finish(tile, jnp.maximum(tile - 1, 0))
        push(jnp.minimum(tile + 1, tiles - 1))

        def per_trip(trip, carry):
            step(tile + 1, trip, tile + 1, trip - 1, False)
            return carry

        lax.fori_loop(1, n_trip, per_trip, 0)
        return carry

    best[0][0] = floor
    best[1][0] = floor
    lax.fori_loop(0, n_tile, per_tile, 0)
    for k in range(LANES):
        for unit in range(2):
            drain(unit, k, n_tile, n_trip - 1)
    finish(n_tile, n_tile - 1)
    for unit in range(2):
        pltpu.matmul_acc_lhs(accs[unit][0], jnp.zeros((UNIT, 256), BF16), load_staged_rhs=0)
        pltpu.matmul_pop(accs[unit][0])


def score_kernel(nd, rows, tiles, table, q_all, p_ext, out, q_list, best0, best1):
    def body(*accs):
        score_body(nd, rows, tiles, table, q_all, p_ext, out, q_list, (best0, best1), (accs[:LANES], accs[LANES:]))

    pl.run_scoped(body, *[pltpu.ACC(0)((UNIT, 256), F32)] * LANES, *[pltpu.ACC(1)((UNIT, 256), F32)] * LANES)


def gather_kernel(nd, tiles, temp, best, seg, scores, send_sem, recv_sem):
    me = place(0)[1]
    barrier = pltpu.get_barrier_semaphore()
    for rel in range(1, 8):
        pl.semaphore_signal(barrier, inc=1, device_id=place(rel)[0], device_id_type=MESH)
    total = jnp.zeros((nd, nd * 8), F32)
    for t in range(tiles):
        value = best[t]
        high = value.astype(BF16)
        rest = value - high.astype(F32)
        mid = rest.astype(BF16)
        low = (rest - mid.astype(F32)).astype(BF16)
        part = dot(jnp.concatenate([high, mid, low], axis=0), seg[t * 256:(t + 1) * 256, :])
        total = total + ((part[0:nd] + part[nd:2 * nd]) + part[2 * nd:3 * nd])
    scores[pl.ds(me * nd, nd), :] = total / temp[0]
    pl.semaphore_wait(barrier, 7)

    def remote(origin_rel, rel):
        block = scores.at[pl.ds(place(origin_rel)[1] * nd, nd)]
        return pltpu.make_async_remote_copy(src_ref=block, dst_ref=block, send_sem=send_sem.at[rel - 1],
                                            recv_sem=recv_sem.at[rel - 1], device_id=place(rel)[0], device_id_type=MESH)

    copies = [remote(0, rel) for rel in (6, 7, 2, 3, 4, 5, 1)]
    for copy in copies:
        copy.start()
    for rel in range(1, 8):
        remote(rel, rel).wait_recv()
    for copy in copies:
        copy.wait_send()


def loss_kernel(nq, scores, losses, mean):
    n = nq * 8
    me = place(0)[1]
    logits = scores[...]
    own = jnp.sum(jnp.where(iota((n, n), 0) == iota((n, n), 1), logits, 0.0), axis=0, keepdims=True)
    peak = jnp.max(logits, axis=0, keepdims=True)
    loss = jnp.log(jnp.sum(jnp.exp(logits - peak), axis=0, keepdims=True)) + peak - own
    mean[...] = jnp.sum(loss, axis=1, keepdims=True) / n
    row, col = iota((nq, n), 0), iota((nq, n), 1)
    picked = jnp.sum(jnp.where(col == me * nq + row, loss, 0.0), axis=1, keepdims=True)
    losses[...] = jnp.sum(jnp.where(col == row, picked, 0.0), axis=0, keepdims=True)[:, 0:nq]


VMEM = pl.BlockSpec(memory_space=pltpu.VMEM)
SMEM = pl.BlockSpec(memory_space=pltpu.SMEM)
ANY = pl.BlockSpec(memory_space=pl.ANY)
DMA = pltpu.SemaphoreType.DMA


def solution(mesh):
    def local_step(query_hidden, doc_hidden, w_proj, query_mask, doc_mask, temperature):
        nq, qlen, hidden = query_hidden.shape
        nd, dlen, _ = doc_hidden.shape
        rows = nq * qlen
        tiles = rows * 8 // 256
        hbm = lambda x: pltpu.with_memory_space_constraint(x, pltpu.HBM)
        vmem = lambda x: pltpu.with_memory_space_constraint(x, pltpu.VMEM)
        q_all, p_head, table, seg, nmt = pl.pallas_call(
            functools.partial(project_kernel, nq, qlen, nd, dlen),
            out_shape=[
                pltpu.VMEM((rows * 8, 128), BF16),
                pltpu.VMEM((nd * dlen, 256), BF16),
                pltpu.VMEM((8, 256), jnp.int32),
                pltpu.VMEM((rows * 8, nq * 8), BF16),
                pltpu.VMEM((dlen, 128), BF16),
            ],
            in_specs=[ANY] * 5,
            out_specs=[VMEM] * 5,
            scratch_shapes=[
                pltpu.VMEM((nq * 8, qlen), jnp.int32),
                pltpu.VMEM((rows, hidden), BF16),
                pltpu.VMEM((hidden, 128), BF16),
                pltpu.VMEM((nd, dlen), jnp.int32),
                pltpu.VMEM((RING, HEAD, hidden), BF16),
                DMA((4,)), DMA((RING,)), DMA((7,)), DMA((7,)), DMA((7,)), DMA((7,)),
            ],
            compiler_params=pltpu.CompilerParams(collective_id=0, has_side_effects=True, vmem_limit_bytes=30 * 2**20),
            name='project',
        )(hbm(query_hidden.reshape(rows, hidden)), hbm(doc_hidden.reshape(nd * dlen, hidden)), hbm(w_proj),
          hbm(query_mask), hbm(doc_mask))

        p_ext = pl.pallas_call(
            functools.partial(tail_kernel, dlen // UNIT),
            out_shape=pltpu.VMEM((nd * dlen, 256), BF16),
            in_specs=[SMEM, ANY, VMEM, VMEM, VMEM],
            out_specs=VMEM,
            scratch_shapes=[pltpu.VMEM((TAIL_RING, GROUP * UNIT, hidden), BF16), DMA((TAIL_RING,))],
            input_output_aliases={4: 0},
            compiler_params=pltpu.CompilerParams(vmem_limit_bytes=30 * 2**20),
            name='tail',
        )(table, hbm(doc_hidden.reshape(nd * dlen, hidden)), w_proj, vmem(nmt), vmem(p_head))

        best = pl.pallas_call(
            functools.partial(score_kernel, nd, rows, tiles),
            out_shape=pltpu.VMEM((tiles, nd, 256), F32),
            in_specs=[SMEM, VMEM, VMEM],
            out_specs=VMEM,
            scratch_shapes=[
                pltpu.VMEM((rows * 8 + 512, 128), BF16),
                pltpu.VMEM((tiles + 1, nd, 8, 256), F32),
                pltpu.VMEM((tiles + 1, nd, 8, 256), F32),
            ],
            compiler_params=pltpu.CompilerParams(vmem_limit_bytes=30 * 2**20),
            name='score',
        )(table, vmem(q_all), vmem(p_ext))

        scores = pl.pallas_call(
            functools.partial(gather_kernel, nd, tiles),
            out_shape=pltpu.VMEM((nd * 8, nq * 8), F32),
            in_specs=[SMEM, VMEM, VMEM],
            out_specs=VMEM,
            scratch_shapes=[DMA((7,)), DMA((7,))],
            compiler_params=pltpu.CompilerParams(collective_id=1, has_side_effects=True),
            name='gather',
        )(temperature.reshape(1), vmem(best), vmem(seg))

        losses, mean = pl.pallas_call(
            functools.partial(loss_kernel, nq),
            out_shape=[jax.ShapeDtypeStruct((1, nq), F32), jax.ShapeDtypeStruct((1, 1), F32)],
            in_specs=[VMEM],
            out_specs=[VMEM, VMEM],
            name='loss',
        )(vmem(scores))
        return losses.reshape(nq), mean.reshape(1)

    tok, mask, row = P(('replica', 'data2', 'data'), None, None), P(('replica', 'data2', 'data'), None), P(('replica', 'data2', 'data'))
    return jax.shard_map(local_step, mesh=mesh, in_specs=(tok, tok, P(None, None), mask, mask, P()),
                         out_specs=(row, P('replica')), check_vma=False)
```

```python
import functools

import jax
import jax.numpy as jnp
from jax import lax
from jax.experimental import pallas as pl
from jax.experimental.pallas import tpu as pltpu
from jax.sharding import PartitionSpec as P

MESH = pl.DeviceIdType.MESH
F32, BF16 = jnp.float32, jnp.bfloat16
BIG = 1e30
UNIT = 64
LANES = 8
RING = 3
HEAD = 448
GROUP = 4
TAIL_RING = 8


def iota(shape, dim):
    return lax.broadcasted_iota(jnp.int32, shape, dim)


def dot(a, b):
    return jnp.dot(a, b, preferred_element_type=F32)


def place(rel):
    y, d = lax.axis_index('data2'), lax.axis_index('data')
    x, core = d // 2, d % 2
    y = 1 - y if rel & 4 else y
    x = 1 - x if rel & 2 else x
    core = 1 - core if rel & 1 else core
    return {'data2': y, 'data': x * 2 + core}, y * 4 + x * 2 + core


def unit_rows(projected):
    square = jnp.sum(projected * projected, axis=-1, keepdims=True)
    return (projected * lax.rsqrt(jnp.maximum(square, 1e-24))).astype(BF16)


def mask_features(doc, off):
    return jnp.where(iota(off.shape, 1) == doc, off.astype(F32), 0.0).astype(BF16)


def project_kernel(nq, qlen, nd, dlen, q_hbm, d_hbm, w_hbm, qm_hbm, dm_hbm, q_all, p_ext, table, seg, nmt,
                   qm_all, q_buf, w_buf, dm_buf, d_buf, in_sem, d_sem, qs_sem, qr_sem, ms_sem, mr_sem):
    rows = nq * qlen
    n = nq * 8
    me = place(0)[1]
    as_bf = lambda cond: cond.astype(F32).astype(BF16)
    ins = [pltpu.make_async_copy(src, dst, in_sem.at[k]) for k, (src, dst) in enumerate(
        [(qm_hbm, qm_all.at[pl.ds(me * nq, nq)]), (dm_hbm, dm_buf), (w_hbm, w_buf), (q_hbm, q_buf)])]
    for copy in ins:
        copy.start()

    def doc_copy(j, slot):
        return pltpu.make_async_copy(d_hbm.at[pl.ds(j * dlen, HEAD)], d_buf.at[slot], d_sem.at[slot])

    for j in range(RING):
        doc_copy(j, j).start()

    barrier = pltpu.get_barrier_semaphore()
    for rel in range(1, 8):
        pl.semaphore_signal(barrier, inc=1, device_id=place(rel)[0], device_id_type=MESH)

    def remote(ref, per, origin_rel, to_rel, send_sem, recv_sem):
        block = ref.at[pl.ds(place(origin_rel)[1] * per, per)]
        return pltpu.make_async_remote_copy(src_ref=block, dst_ref=block, send_sem=send_sem, recv_sem=recv_sem,
                                            device_id=place(to_rel)[0], device_id_type=MESH)

    ins[0].wait()
    pl.semaphore_wait(barrier, 7)
    mask_sent = [remote(qm_all, nq, 0, rel, ms_sem.at[rel - 1], mr_sem.at[rel - 1]) for rel in (6, 7, 2, 3, 4, 5, 1)]
    for copy in mask_sent:
        copy.start()

    mask = qm_all[pl.ds(me * nq, nq), :].astype(F32).astype(BF16)
    spread = dot(mask, as_bf(iota((qlen, rows), 1) % qlen == iota((qlen, rows), 0)))
    flat = jnp.sum(jnp.where(iota((nq, rows), 1) // qlen == iota((nq, rows), 0), spread, 0.0), axis=0, keepdims=True)
    before = as_bf(iota((rows, rows), 0) < iota((rows, rows), 1))
    rank = dot(jnp.broadcast_to(flat, (16, rows)).astype(BF16), before)[0:1]
    rank = jnp.where(flat > 0.5, rank, -1.0).astype(jnp.int32)
    pick = as_bf(iota((rows, rows), 0) == rank)

    ins[2].wait()
    ins[3].wait()
    q_vec = unit_rows(dot(q_buf[...], w_buf[...]))
    q_all[pl.ds(me * rows, rows), :] = dot(pick, q_vec).astype(BF16)
    sent = []

    def send(origin_rel, to_rel):
        copy = remote(q_all, rows, origin_rel, to_rel, qs_sem.at[len(sent)], qr_sem.at[(origin_rel ^ to_rel) - 1])
        copy.start()
        sent.append(copy)

    def received(rel):
        remote(q_all, rows, rel, rel, qs_sem.at[0], qr_sem.at[rel - 1]).wait_recv()

    for rel in (2, 4, 6, 1):
        send(0, rel)

    ins[1].wait()
    dmask = dm_buf[...]
    off = jnp.concatenate([1.0 - dmask.astype(F32), jnp.zeros((128 - nd, dlen), F32)], axis=0)
    nmt[...] = jnp.transpose(off).astype(BF16)
    last = jnp.max(dmask * (iota((nd, dlen), 1) + 1), axis=1, keepdims=True).astype(F32)
    per_doc = dlen // UNIT
    count = jnp.floor((last + (UNIT - 1.0)) * (1.0 / UNIT))
    sums = as_bf(iota((nd, nd), 0) >= iota((nd, nd), 1))

    def listing(at, count, first):
        upto = dot(sums, jnp.broadcast_to(count, (nd, 128)).astype(BF16))[:, 0:1]
        total = jnp.max(upto, axis=0, keepdims=True)
        slot_id = jnp.minimum(iota((nd, 256), 1).astype(F32), jnp.maximum(total - 1.0, 0.0))
        passed = slot_id >= upto
        unit = slot_id[0:1] + first + jnp.sum(jnp.where(passed, per_doc - count, 0.0), axis=0, keepdims=True)
        doc = jnp.sum(jnp.where(passed, 1.0, 0.0), axis=0, keepdims=True)
        table[at:at + 1, :] = unit.astype(jnp.int32)
        table[at + 1:at + 2, :] = doc.astype(jnp.int32)
        table[at + 2:at + 3, :] = jnp.broadcast_to(total, (1, 256)).astype(jnp.int32)

    listing(0, count, 0.0)
    listing(4, jnp.maximum(count - HEAD // UNIT, 0.0), float(HEAD // UNIT))

    def project(j, carry):
        slot = lax.rem(j, RING)
        doc_copy(j, slot).wait()
        p_ext[pl.ds(j * dlen, HEAD), 0:128] = unit_rows(dot(d_buf[slot], w_buf[...]))
        p_ext[pl.ds(j * dlen, HEAD), 128:256] = mask_features(j, nmt[0:HEAD, :])

        @pl.when(j + RING < nd)
        def _():
            doc_copy(j + RING, slot).start()

        return carry

    cut1, cut2 = (7 * nd) // 16, (12 * nd) // 16
    lax.fori_loop(0, cut1, project, 0)
    for rel in (2, 4):
        received(rel)
        send(rel, 1)

    for rel in range(1, 8):
        remote(qm_all, nq, rel, rel, ms_sem.at[rel - 1], mr_sem.at[rel - 1]).wait_recv()
    row, col = iota((n, n), 0), iota((n, n), 1)
    every = qm_all[...].astype(F32).astype(BF16)
    counts = lax.dot_general(jnp.ones((16, qlen), BF16), every, (((1,), (1,)), ((), ())), preferred_element_type=F32)
    counts_bf = counts.astype(BF16)
    in_dev = dot(counts_bf, as_bf((row // nq == col // nq) & (row < col)))
    padded = jnp.floor((dot(counts_bf, as_bf(row // nq == col // nq)) + 15.0) * (1.0 / 16.0)) * 16.0
    padded_bf = padded.astype(BF16)
    begin = dot(padded_bf, as_bf((row // nq < col // nq) & (row % nq == 0))) + in_dev
    starts = dot(padded_bf, as_bf((row // nq < col) & (row % nq == 0)))
    table[3:4, 0:128] = starts[0:1].astype(jnp.int32)
    table[3:4, 128:256] = starts[0:1].astype(jnp.int32)
    first = begin[0:1].astype(jnp.int32)
    end = (begin + counts)[0:1].astype(jnp.int32)
    where = iota((rows * 8, n), 0)
    seg[...] = as_bf((where >= first) & (where < end))

    lax.fori_loop(cut1, cut2, project, 0)
    received(6)
    send(6, 1)
    lax.fori_loop(cut2, nd, project, 0)
    for rel in (1, 3, 5, 7):
        received(rel)
    for copy in mask_sent + sent:
        copy.wait_send()


def tail_kernel(per_doc, table, d_hbm, w, nmt, p_head, p_ext, d_buf, sem):
    steps = (table[6, 0] + (GROUP - 1)) // GROUP

    def copies(g):
        slot = lax.rem(g, TAIL_RING)
        return [pltpu.make_async_copy(d_hbm.at[pl.ds(pl.multiple_of(table[4, g * GROUP + k] * UNIT, UNIT), UNIT)],
                                      d_buf.at[slot, pl.ds(k * UNIT, UNIT)], sem.at[slot]) for k in range(GROUP)]

    for g in range(TAIL_RING):
        @pl.when(g < steps)
        def _():
            for k, copy in enumerate(copies(g)):
                copy.start(priority=k % 2)

    def step(g, carry):
        for copy in copies(g):
            copy.wait()
        value = unit_rows(dot(d_buf[lax.rem(g, TAIL_RING)], w[...]))
        for k in range(GROUP):
            unit, doc = table[4, g * GROUP + k], table[5, g * GROUP + k]
            at = pl.ds(pl.multiple_of(unit * UNIT, UNIT), UNIT)
            p_ext[at, 0:128] = value[k * UNIT:(k + 1) * UNIT]
            p_ext[at, 128:256] = mask_features(doc, nmt[pl.ds(pl.multiple_of((unit - doc * per_doc) * UNIT, UNIT), UNIT), :])

        @pl.when(g + TAIL_RING < steps)
        def _():
            for k, copy in enumerate(copies(g + TAIL_RING)):
                copy.start(priority=k % 2)

        return carry

    lax.fori_loop(0, steps, step, 0)


def score_body(nd, rows, tiles, table, q_all, p_ext, out, q_list, best, accs):
    floor = jnp.full((nd, 8, 256), -3e38, F32)
    out[...] = jnp.zeros_like(out)
    for dev in range(8):
        q_list[pl.ds(pl.multiple_of(table[3, dev], 16), rows), :] = q_all[dev * rows:(dev + 1) * rows, :]
    q_list[pl.ds(pl.multiple_of(table[3, 7], 16) + rows, 256), :] = jnp.zeros((256, 128), BF16)
    n_tile = (table[3, 8] + 255) // 256
    n_trip = (table[2, 0] + (2 * LANES - 1)) // (2 * LANES)
    away = jnp.full((256, 128), -BIG, BF16)

    def push(tile):
        q_tile = q_list[pl.ds(pl.multiple_of(tile * 256, 256), 256), :]
        rhs = jnp.concatenate([q_tile, away], axis=1)
        for unit in range(2):
            pltpu.matmul_push_rhs(rhs, staging_register=0, mxu_index=unit, transpose=True)

    def drain(unit, k, slot, trip):
        value = pltpu.matmul_pop(accs[unit][k])
        top = value[0:8]
        for r in range(1, UNIT // 8):
            top = jnp.maximum(top, value[8 * r:8 * r + 8])
        doc = table[1, trip * (2 * LANES) + 2 * k + unit]
        best[unit][slot, doc] = jnp.maximum(best[unit][slot, doc], top)

    def step(slot, trip, prev_slot, prev_trip, first):
        for k in range(LANES):
            for unit in range(2):
                drain(unit, k, prev_slot, prev_trip)
                row = table[0, trip * (2 * LANES) + 2 * k + unit] * UNIT
                lhs = p_ext[pl.ds(pl.multiple_of(row, UNIT), UNIT), :]
                pltpu.matmul_acc_lhs(accs[unit][k], lhs, load_staged_rhs=0 if first and k == 0 else None)

    def finish(slot, tile):
        both = jnp.maximum(best[0][slot], best[1][slot])
        out[tile] = jnp.max(both, axis=1)

    for unit in range(2):
        for k in range(LANES):
            pltpu.matmul_pop(accs[unit][k])
    push(0)

    def per_tile(tile, carry):
        best[0][tile + 1] = floor
        best[1][tile + 1] = floor
        step(tile + 1, 0, tile, n_trip - 1, True)
        finish(tile, jnp.maximum(tile - 1, 0))
        push(jnp.minimum(tile + 1, tiles - 1))

        def per_trip(trip, carry):
            step(tile + 1, trip, tile + 1, trip - 1, False)
            return carry

        lax.fori_loop(1, n_trip, per_trip, 0)
        return carry

    best[0][0] = floor
    best[1][0] = floor
    lax.fori_loop(0, n_tile, per_tile, 0)
    for k in range(LANES):
        for unit in range(2):
            drain(unit, k, n_tile, n_trip - 1)
    finish(n_tile, n_tile - 1)
    for unit in range(2):
        pltpu.matmul_acc_lhs(accs[unit][0], jnp.zeros((UNIT, 256), BF16), load_staged_rhs=0)
        pltpu.matmul_pop(accs[unit][0])


def score_kernel(nd, rows, tiles, table, q_all, p_ext, out, q_list, best0, best1):
    def body(*accs):
        score_body(nd, rows, tiles, table, q_all, p_ext, out, q_list, (best0, best1), (accs[:LANES], accs[LANES:]))

    pl.run_scoped(body, *[pltpu.ACC(0)((UNIT, 256), F32)] * LANES, *[pltpu.ACC(1)((UNIT, 256), F32)] * LANES)


def gather_kernel(nd, tiles, temp, best, seg, scores, send_sem, recv_sem):
    me = place(0)[1]
    barrier = pltpu.get_barrier_semaphore()
    for rel in range(1, 8):
        pl.semaphore_signal(barrier, inc=1, device_id=place(rel)[0], device_id_type=MESH)
    total = jnp.zeros((nd, nd * 8), F32)
    for t in range(tiles):
        value = best[t]
        high = value.astype(BF16)
        rest = value - high.astype(F32)
        mid = rest.astype(BF16)
        low = (rest - mid.astype(F32)).astype(BF16)
        part = dot(jnp.concatenate([high, mid, low], axis=0), seg[t * 256:(t + 1) * 256, :])
        total = total + ((part[0:nd] + part[nd:2 * nd]) + part[2 * nd:3 * nd])
    scores[pl.ds(me * nd, nd), :] = total / temp[0]
    pl.semaphore_wait(barrier, 7)

    def remote(origin_rel, rel):
        block = scores.at[pl.ds(place(origin_rel)[1] * nd, nd)]
        return pltpu.make_async_remote_copy(src_ref=block, dst_ref=block, send_sem=send_sem.at[rel - 1],
                                            recv_sem=recv_sem.at[rel - 1], device_id=place(rel)[0], device_id_type=MESH)

    copies = [remote(0, rel) for rel in (6, 7, 2, 3, 4, 5, 1)]
    for copy in copies:
        copy.start()
    for rel in range(1, 8):
        remote(rel, rel).wait_recv()
    for copy in copies:
        copy.wait_send()


def loss_kernel(nq, scores, losses, mean):
    n = nq * 8
    me = place(0)[1]
    logits = scores[...]
    own = jnp.sum(jnp.where(iota((n, n), 0) == iota((n, n), 1), logits, 0.0), axis=0, keepdims=True)
    peak = jnp.max(logits, axis=0, keepdims=True)
    loss = jnp.log(jnp.sum(jnp.exp(logits - peak), axis=0, keepdims=True)) + peak - own
    mean[...] = jnp.sum(loss, axis=1, keepdims=True) / n
    row, col = iota((nq, n), 0), iota((nq, n), 1)
    picked = jnp.sum(jnp.where(col == me * nq + row, loss, 0.0), axis=1, keepdims=True)
    losses[...] = jnp.sum(jnp.where(col == row, picked, 0.0), axis=0, keepdims=True)[:, 0:nq]


VMEM = pl.BlockSpec(memory_space=pltpu.VMEM)
SMEM = pl.BlockSpec(memory_space=pltpu.SMEM)
ANY = pl.BlockSpec(memory_space=pl.ANY)
DMA = pltpu.SemaphoreType.DMA


def solution(mesh):
    def local_step(query_hidden, doc_hidden, w_proj, query_mask, doc_mask, temperature):
        nq, qlen, hidden = query_hidden.shape
        nd, dlen, _ = doc_hidden.shape
        rows = nq * qlen
        tiles = rows * 8 // 256
        hbm = lambda x: pltpu.with_memory_space_constraint(x, pltpu.HBM)
        vmem = lambda x: pltpu.with_memory_space_constraint(x, pltpu.VMEM)
        q_all, p_head, table, seg, nmt = pl.pallas_call(
            functools.partial(project_kernel, nq, qlen, nd, dlen),
            out_shape=[
                pltpu.VMEM((rows * 8, 128), BF16),
                pltpu.VMEM((nd * dlen, 256), BF16),
                pltpu.VMEM((8, 256), jnp.int32),
                pltpu.VMEM((rows * 8, nq * 8), BF16),
                pltpu.VMEM((dlen, 128), BF16),
            ],
            in_specs=[ANY] * 5,
            out_specs=[VMEM] * 5,
            scratch_shapes=[
                pltpu.VMEM((nq * 8, qlen), jnp.int32),
                pltpu.VMEM((rows, hidden), BF16),
                pltpu.VMEM((hidden, 128), BF16),
                pltpu.VMEM((nd, dlen), jnp.int32),
                pltpu.VMEM((RING, HEAD, hidden), BF16),
                DMA((4,)), DMA((RING,)), DMA((7,)), DMA((7,)), DMA((7,)), DMA((7,)),
            ],
            compiler_params=pltpu.CompilerParams(collective_id=0, has_side_effects=True, vmem_limit_bytes=30 * 2**20),
            name='project',
        )(hbm(query_hidden.reshape(rows, hidden)), hbm(doc_hidden.reshape(nd * dlen, hidden)), hbm(w_proj),
          hbm(query_mask), hbm(doc_mask))

        p_ext = pl.pallas_call(
            functools.partial(tail_kernel, dlen // UNIT),
            out_shape=pltpu.VMEM((nd * dlen, 256), BF16),
            in_specs=[SMEM, ANY, VMEM, VMEM, VMEM],
            out_specs=VMEM,
            scratch_shapes=[pltpu.VMEM((TAIL_RING, GROUP * UNIT, hidden), BF16), DMA((TAIL_RING,))],
            input_output_aliases={4: 0},
            compiler_params=pltpu.CompilerParams(vmem_limit_bytes=30 * 2**20),
            name='tail',
        )(table, hbm(doc_hidden.reshape(nd * dlen, hidden)), w_proj, vmem(nmt), vmem(p_head))

        best = pl.pallas_call(
            functools.partial(score_kernel, nd, rows, tiles),
            out_shape=pltpu.VMEM((tiles, nd, 256), F32),
            in_specs=[SMEM, VMEM, VMEM],
            out_specs=VMEM,
            scratch_shapes=[
                pltpu.VMEM((rows * 8 + 512, 128), BF16),
                pltpu.VMEM((tiles + 1, nd, 8, 256), F32),
                pltpu.VMEM((tiles + 1, nd, 8, 256), F32),
            ],
            compiler_params=pltpu.CompilerParams(vmem_limit_bytes=30 * 2**20),
            name='score',
        )(table, vmem(q_all), vmem(p_ext))

        scores = pl.pallas_call(
            functools.partial(gather_kernel, nd, tiles),
            out_shape=pltpu.VMEM((nd * 8, nq * 8), F32),
            in_specs=[SMEM, VMEM, VMEM],
            out_specs=VMEM,
            scratch_shapes=[DMA((7,)), DMA((7,))],
            compiler_params=pltpu.CompilerParams(collective_id=1, has_side_effects=True),
            name='gather',
        )(temperature.reshape(1), vmem(best), vmem(seg))

        losses, mean = pl.pallas_call(
            functools.partial(loss_kernel, nq),
            out_shape=[jax.ShapeDtypeStruct((1, nq), F32), jax.ShapeDtypeStruct((1, 1), F32)],
            in_specs=[VMEM],
            out_specs=[VMEM, VMEM],
            name='loss',
        )(vmem(scores))
        return losses.reshape(nq), mean.reshape(1)

    tok, mask, row = P(('replica', 'data2', 'data'), None, None), P(('replica', 'data2', 'data'), None), P(('replica', 'data2', 'data'))
    return jax.shard_map(local_step, mesh=mesh, in_specs=(tok, tok, P(None, None), mask, mask, P()),
                         out_specs=(row, P('replica')), check_vma=False)
```

```python
import functools

import jax
import jax.numpy as jnp
from jax import lax
from jax.experimental import pallas as pl
from jax.experimental.pallas import tpu as pltpu
from jax.sharding import PartitionSpec as P

MESH = pl.DeviceIdType.MESH
F32, BF16 = jnp.float32, jnp.bfloat16
BIG = 1e30
UNIT = 64
LANES = 8
RING = 4
HEAD = 256
GROUP = 16


def iota(shape, dim):
    return lax.broadcasted_iota(jnp.int32, shape, dim)


def dot(a, b):
    return jnp.dot(a, b, preferred_element_type=F32)


def place(rel):
    y, d = lax.axis_index('data2'), lax.axis_index('data')
    x, core = d // 2, d % 2
    y = 1 - y if rel & 4 else y
    x = 1 - x if rel & 2 else x
    core = 1 - core if rel & 1 else core
    return {'data2': y, 'data': x * 2 + core}, y * 4 + x * 2 + core


def unit_rows(projected):
    square = jnp.sum(projected * projected, axis=-1, keepdims=True)
    return (projected * lax.rsqrt(jnp.maximum(square, 1e-24))).astype(BF16)


def mask_features(doc, off):
    return jnp.where(iota(off.shape, 1) == doc, off.astype(F32), 0.0).astype(BF16)


def project_kernel(nq, qlen, nd, dlen, q_hbm, d_hbm, w_hbm, qm_hbm, dm_hbm, q_all, p_ext, table, seg, nmt,
                   qm_all, q_buf, w_buf, dm_buf, d_buf, in_sem, d_sem, qs_sem, qr_sem, ms_sem, mr_sem):
    rows = nq * qlen
    n = nq * 8
    me = place(0)[1]
    as_bf = lambda cond: cond.astype(F32).astype(BF16)
    ins = [pltpu.make_async_copy(src, dst, in_sem.at[k]) for k, (src, dst) in enumerate(
        [(qm_hbm, qm_all.at[pl.ds(me * nq, nq)]), (dm_hbm, dm_buf), (w_hbm, w_buf), (q_hbm, q_buf)])]
    for copy in ins:
        copy.start()

    def doc_copy(j, slot):
        return pltpu.make_async_copy(d_hbm.at[pl.ds(j * dlen, HEAD)], d_buf.at[slot], d_sem.at[slot])

    for j in range(RING):
        doc_copy(j, j).start()

    barrier = pltpu.get_barrier_semaphore()
    for rel in range(1, 8):
        pl.semaphore_signal(barrier, inc=1, device_id=place(rel)[0], device_id_type=MESH)

    def remote(ref, per, origin_rel, to_rel, send_sem, recv_sem):
        block = ref.at[pl.ds(place(origin_rel)[1] * per, per)]
        return pltpu.make_async_remote_copy(src_ref=block, dst_ref=block, send_sem=send_sem, recv_sem=recv_sem,
                                            device_id=place(to_rel)[0], device_id_type=MESH)

    ins[0].wait()
    pl.semaphore_wait(barrier, 7)
    mask_sent = [remote(qm_all, nq, 0, rel, ms_sem.at[rel - 1], mr_sem.at[rel - 1]) for rel in (6, 7, 2, 3, 4, 5, 1)]
    for copy in mask_sent:
        copy.start()

    mask = qm_all[pl.ds(me * nq, nq), :].astype(F32).astype(BF16)
    spread = dot(mask, as_bf(iota((qlen, rows), 1) % qlen == iota((qlen, rows), 0)))
    flat = jnp.sum(jnp.where(iota((nq, rows), 1) // qlen == iota((nq, rows), 0), spread, 0.0), axis=0, keepdims=True)
    before = as_bf(iota((rows, rows), 0) < iota((rows, rows), 1))
    rank = dot(jnp.broadcast_to(flat, (16, rows)).astype(BF16), before)[0:1]
    rank = jnp.where(flat > 0.5, rank, -1.0).astype(jnp.int32)
    pick = as_bf(iota((rows, rows), 0) == rank)

    ins[2].wait()
    ins[3].wait()
    q_vec = unit_rows(dot(q_buf[...], w_buf[...]))
    q_all[pl.ds(me * rows, rows), :] = dot(pick, q_vec).astype(BF16)
    sent = []

    def send(origin_rel, to_rel):
        copy = remote(q_all, rows, origin_rel, to_rel, qs_sem.at[len(sent)], qr_sem.at[(origin_rel ^ to_rel) - 1])
        copy.start()
        sent.append(copy)

    def received(rel):
        remote(q_all, rows, rel, rel, qs_sem.at[0], qr_sem.at[rel - 1]).wait_recv()

    for rel in (2, 4, 6, 1):
        send(0, rel)

    ins[1].wait()
    dmask = dm_buf[...]
    off = jnp.concatenate([1.0 - dmask.astype(F32), jnp.zeros((128 - nd, dlen), F32)], axis=0)
    nmt[...] = jnp.transpose(off).astype(BF16)
    last = jnp.max(dmask * (iota((nd, dlen), 1) + 1), axis=1, keepdims=True).astype(F32)
    count = jnp.floor((last + (UNIT - 1.0)) * (1.0 / UNIT))
    sums = as_bf(iota((nd, nd), 0) >= iota((nd, nd), 1))

    def listing(at, count, per, first):
        upto = dot(sums, jnp.broadcast_to(count, (nd, 128)).astype(BF16))[:, 0:1]
        total = jnp.max(upto, axis=0, keepdims=True)
        slot_id = jnp.minimum(iota((nd, 256), 1).astype(F32), jnp.maximum(total - 1.0, 0.0))
        passed = slot_id >= upto
        unit = slot_id[0:1] + first + jnp.sum(jnp.where(passed, per - count, 0.0), axis=0, keepdims=True)
        doc = jnp.sum(jnp.where(passed, 1.0, 0.0), axis=0, keepdims=True)
        table[at:at + 1, :] = unit.astype(jnp.int32)
        table[at + 1:at + 2, :] = doc.astype(jnp.int32)
        table[at + 2:at + 3, :] = jnp.broadcast_to(total, (1, 256)).astype(jnp.int32)

    head = float(HEAD // UNIT)
    listing(0, jnp.minimum(count, head), head, 0.0)
    listing(4, jnp.maximum(count - head, 0.0), float(dlen // UNIT), head)

    def project(j, carry):
        slot = lax.rem(j, RING)
        doc_copy(j, slot).wait()
        p_ext[pl.ds(j * HEAD, HEAD), 0:128] = unit_rows(dot(d_buf[slot], w_buf[...]))
        p_ext[pl.ds(j * HEAD, HEAD), 128:256] = mask_features(j, nmt[0:HEAD, :])

        @pl.when(j + RING < nd)
        def _():
            doc_copy(j + RING, slot).start()

        return carry

    cut = (13 * nd) // 16
    lax.fori_loop(0, cut, project, 0)
    for rel in (2, 4):
        received(rel)
        send(rel, 1)
    lax.fori_loop(cut, nd, project, 0)

    for rel in range(1, 8):
        remote(qm_all, nq, rel, rel, ms_sem.at[rel - 1], mr_sem.at[rel - 1]).wait_recv()
    row, col = iota((n, n), 0), iota((n, n), 1)
    every = qm_all[...].astype(F32).astype(BF16)
    counts = lax.dot_general(jnp.ones((16, qlen), BF16), every, (((1,), (1,)), ((), ())), preferred_element_type=F32)
    counts_bf = counts.astype(BF16)
    in_dev = dot(counts_bf, as_bf((row // nq == col // nq) & (row < col)))
    padded = jnp.floor((dot(counts_bf, as_bf(row // nq == col // nq)) + 15.0) * (1.0 / 16.0)) * 16.0
    padded_bf = padded.astype(BF16)
    begin = dot(padded_bf, as_bf((row // nq < col // nq) & (row % nq == 0))) + in_dev
    starts = dot(padded_bf, as_bf((row // nq < col) & (row % nq == 0)))
    table[3:4, 0:128] = starts[0:1].astype(jnp.int32)
    table[3:4, 128:256] = starts[0:1].astype(jnp.int32)
    first = begin[0:1].astype(jnp.int32)
    end = (begin + counts)[0:1].astype(jnp.int32)
    where = iota((rows * 8, n), 0)
    seg[...] = as_bf((where >= first) & (where < end))

    received(6)
    send(6, 1)
    for rel in (1, 3, 5, 7):
        received(rel)
    for copy in mask_sent + sent:
        copy.wait_send()


def score_body(nd, rows, tiles, per_doc, hidden, table, q_all, p_head, nmt, w, d_hbm, out, q_list, best, p_tail, d_buf,
               sem, accs):
    n_head, n_tail = table[2, 0], table[6, 0]
    n_group = (n_tail + (GROUP - 1)) // GROUP

    def fetch(g, carry):
        for k in range(GROUP):
            row = pl.multiple_of(table[4, g * GROUP + k] * UNIT, UNIT)
            pltpu.make_async_copy(d_hbm.at[pl.ds(row, UNIT)], d_buf.at[g, pl.ds(k * UNIT, UNIT)],
                                  sem.at[g]).start(priority=k % 2)
        return carry

    lax.fori_loop(0, n_group, fetch, 0)

    floor = jnp.full((nd, 8, 256), -3e38, F32)
    out[...] = jnp.zeros_like(out)
    for dev in range(8):
        q_list[pl.ds(pl.multiple_of(table[3, dev], 16), rows), :] = q_all[dev * rows:(dev + 1) * rows, :]
    q_list[pl.ds(pl.multiple_of(table[3, 7], 16) + rows, 256), :] = jnp.zeros((256, 128), BF16)
    n_tile = (table[3, 8] + 255) // 256
    away = jnp.full((256, 128), -BIG, BF16)

    def push(tile):
        q_tile = q_list[pl.ds(pl.multiple_of(tile * 256, 256), 256), :]
        rhs = jnp.concatenate([q_tile, away], axis=1)
        for unit in range(2):
            pltpu.matmul_push_rhs(rhs, staging_register=0, mxu_index=unit, transpose=True)

    def unstage():
        for unit in range(2):
            pltpu.matmul_acc_lhs(accs[unit][0], jnp.zeros((UNIT, 256), BF16), load_staged_rhs=0)
            pltpu.matmul_pop(accs[unit][0])

    def finish(slot, tile):
        out[tile] = jnp.max(jnp.maximum(best[0][slot], best[1][slot]), axis=1)

    def sweep(at, count, row_of, src, is_last):
        n_trip = (count + (2 * LANES - 1)) // (2 * LANES)
        todo = jnp.where(count > 0, n_tile, 0)

        def drain(unit, k, slot, trip):
            value = pltpu.matmul_pop(accs[unit][k])
            top = value[0:8]
            for r in range(1, UNIT // 8):
                top = jnp.maximum(top, value[8 * r:8 * r + 8])
            doc = table[at + 1, jnp.maximum(trip, 0) * (2 * LANES) + 2 * k + unit]
            best[unit][slot, doc] = jnp.maximum(best[unit][slot, doc], top)

        def step(slot, trip, prev_slot, prev_trip, first):
            for k in range(LANES):
                for unit in range(2):
                    drain(unit, k, prev_slot, prev_trip)
                    row = row_of(trip * (2 * LANES) + 2 * k + unit) * UNIT
                    lhs = src[pl.ds(pl.multiple_of(row, UNIT), UNIT), :]
                    pltpu.matmul_acc_lhs(accs[unit][k], lhs, load_staged_rhs=0 if first and k == 0 else None)

        push(0)

        def per_tile(tile, carry):
            if not is_last:
                best[0][tile + 1] = floor
                best[1][tile + 1] = floor
            step(tile + 1, 0, tile, n_trip - 1, True)
            if is_last:
                finish(tile, jnp.maximum(tile - 1, 0))
            push(jnp.minimum(tile + 1, tiles - 1))

            def per_trip(trip, carry):
                step(tile + 1, trip, tile + 1, trip - 1, False)
                return carry

            lax.fori_loop(1, n_trip, per_trip, 0)
            return carry

        lax.fori_loop(0, todo, per_tile, 0)
        for k in range(LANES):
            for unit in range(2):
                drain(unit, k, todo, n_trip - 1)
        unstage()

    for unit in range(2):
        best[unit][0] = floor
        for k in range(LANES):
            pltpu.matmul_pop(accs[unit][k])
    sweep(0, n_head, lambda i: table[0, i], p_head, False)

    depth = hidden // 256
    blank = jnp.zeros((256, 128), BF16)

    def push_w(k):
        rhs = jnp.concatenate([w[k * 256:(k + 1) * 256, :], blank], axis=1)
        for unit in range(2):
            pltpu.matmul_push_rhs(rhs, staging_register=0, mxu_index=unit, transpose=False)

    push_w(0)

    def project(g, carry):
        pltpu.make_async_copy(d_hbm.at[pl.ds(0, GROUP * UNIT)], d_buf.at[g], sem.at[g]).wait()
        for half in range(2):
            for k in range(depth):
                for q in range(4):
                    for unit in range(2):
                        at = (half * 8 + unit * 4 + q) * UNIT
                        pltpu.matmul_acc_lhs(accs[unit][half * 4 + q],
                                             d_buf[g, at:at + UNIT, k * 256:(k + 1) * 256],
                                             load_staged_rhs=0 if q == 0 else None)
                push_w((k + 1) % depth)
            for q in range(4):
                for unit in range(2):
                    index = g * GROUP + half * 8 + unit * 4 + q
                    value = pltpu.matmul_pop(accs[unit][half * 4 + q])[:, 0:128]
                    dst = pl.ds(pl.multiple_of(index * UNIT, UNIT), UNIT)
                    doc = table[5, index]
                    off = nmt[pl.ds(pl.multiple_of((table[4, index] - doc * per_doc) * UNIT, UNIT), UNIT), :]
                    p_tail[dst, 0:128] = unit_rows(value)
                    p_tail[dst, 128:256] = mask_features(doc, off)
        return carry

    lax.fori_loop(0, n_group, project, 0)
    unstage()

    sweep(4, n_tail, lambda i: jnp.minimum(i, n_tail - 1), p_tail, True)

    def finish_all(tile, carry):
        finish(tile + 1, tile)
        return carry

    lax.fori_loop(jnp.where(n_tail > 0, n_tile - 1, 0), n_tile, finish_all, 0)


def score_kernel(nd, rows, tiles, per_doc, hidden, table, q_all, p_head, nmt, w, d_hbm, out, q_list, best0, best1, p_tail,
                 d_buf, sem):
    def body(*accs):
        score_body(nd, rows, tiles, per_doc, hidden, table, q_all, p_head, nmt, w, d_hbm, out, q_list, (best0, best1),
                   p_tail, d_buf, sem, (accs[:LANES], accs[LANES:]))

    pl.run_scoped(body, *[pltpu.ACC(0)((UNIT, 256), F32)] * LANES, *[pltpu.ACC(1)((UNIT, 256), F32)] * LANES)


def gather_kernel(nd, tiles, temp, best, seg, scores, send_sem, recv_sem):
    me = place(0)[1]
    barrier = pltpu.get_barrier_semaphore()
    for rel in range(1, 8):
        pl.semaphore_signal(barrier, inc=1, device_id=place(rel)[0], device_id_type=MESH)
    total = jnp.zeros((nd, nd * 8), F32)
    for t in range(tiles):
        value = best[t]
        high = value.astype(BF16)
        rest = value - high.astype(F32)
        mid = rest.astype(BF16)
        low = (rest - mid.astype(F32)).astype(BF16)
        part = dot(jnp.concatenate([high, mid, low], axis=0), seg[t * 256:(t + 1) * 256, :])
        total = total + ((part[0:nd] + part[nd:2 * nd]) + part[2 * nd:3 * nd])
    scores[pl.ds(me * nd, nd), :] = total / temp[0]
    pl.semaphore_wait(barrier, 7)

    def remote(origin_rel, rel):
        block = scores.at[pl.ds(place(origin_rel)[1] * nd, nd)]
        return pltpu.make_async_remote_copy(src_ref=block, dst_ref=block, send_sem=send_sem.at[rel - 1],
                                            recv_sem=recv_sem.at[rel - 1], device_id=place(rel)[0], device_id_type=MESH)

    copies = [remote(0, rel) for rel in (6, 7, 2, 3, 4, 5, 1)]
    for copy in copies:
        copy.start()
    for rel in range(1, 8):
        remote(rel, rel).wait_recv()
    for copy in copies:
        copy.wait_send()


def loss_kernel(nq, scores, losses, mean):
    n = nq * 8
    me = place(0)[1]
    logits = scores[...]
    own = jnp.sum(jnp.where(iota((n, n), 0) == iota((n, n), 1), logits, 0.0), axis=0, keepdims=True)
    peak = jnp.max(logits, axis=0, keepdims=True)
    loss = jnp.log(jnp.sum(jnp.exp(logits - peak), axis=0, keepdims=True)) + peak - own
    mean[...] = jnp.sum(loss, axis=1, keepdims=True) / n
    row, col = iota((nq, n), 0), iota((nq, n), 1)
    picked = jnp.sum(jnp.where(col == me * nq + row, loss, 0.0), axis=1, keepdims=True)
    losses[...] = jnp.sum(jnp.where(col == row, picked, 0.0), axis=0, keepdims=True)[:, 0:nq]


VMEM = pl.BlockSpec(memory_space=pltpu.VMEM)
SMEM = pl.BlockSpec(memory_space=pltpu.SMEM)
ANY = pl.BlockSpec(memory_space=pl.ANY)
DMA = pltpu.SemaphoreType.DMA


def solution(mesh):
    def local_step(query_hidden, doc_hidden, w_proj, query_mask, doc_mask, temperature):
        nq, qlen, hidden = query_hidden.shape
        nd, dlen, _ = doc_hidden.shape
        rows = nq * qlen
        tiles = rows * 8 // 256
        hbm = lambda x: pltpu.with_memory_space_constraint(x, pltpu.HBM)
        vmem = lambda x: pltpu.with_memory_space_constraint(x, pltpu.VMEM)
        q_all, p_head, table, seg, nmt = pl.pallas_call(
            functools.partial(project_kernel, nq, qlen, nd, dlen),
            out_shape=[
                pltpu.VMEM((rows * 8, 128), BF16),
                pltpu.VMEM((nd * HEAD, 256), BF16),
                pltpu.VMEM((8, 256), jnp.int32),
                pltpu.VMEM((rows * 8, nq * 8), BF16),
                pltpu.VMEM((dlen, 128), BF16),
            ],
            in_specs=[ANY] * 5,
            out_specs=[VMEM] * 5,
            scratch_shapes=[
                pltpu.VMEM((nq * 8, qlen), jnp.int32),
                pltpu.VMEM((rows, hidden), BF16),
                pltpu.VMEM((hidden, 128), BF16),
                pltpu.VMEM((nd, dlen), jnp.int32),
                pltpu.VMEM((RING, HEAD, hidden), BF16),
                DMA((4,)), DMA((RING,)), DMA((7,)), DMA((7,)), DMA((7,)), DMA((7,)),
            ],
            compiler_params=pltpu.CompilerParams(collective_id=0, has_side_effects=True, vmem_limit_bytes=30 * 2**20),
            name='project',
        )(hbm(query_hidden.reshape(rows, hidden)), hbm(doc_hidden.reshape(nd * dlen, hidden)), hbm(w_proj),
          hbm(query_mask), hbm(doc_mask))

        tail_rows = nd * (dlen - HEAD)
        groups = tail_rows // (GROUP * UNIT)
        best = pl.pallas_call(
            functools.partial(score_kernel, nd, rows, tiles, dlen // UNIT, hidden),
            out_shape=pltpu.VMEM((tiles, nd, 256), F32),
            in_specs=[SMEM, VMEM, VMEM, VMEM, VMEM, ANY],
            out_specs=VMEM,
            scratch_shapes=[
                pltpu.VMEM((rows * 8 + 512, 128), BF16),
                pltpu.VMEM((tiles + 1, nd, 8, 256), F32),
                pltpu.VMEM((tiles + 1, nd, 8, 256), F32),
                pltpu.VMEM((tail_rows, 256), BF16),
                pltpu.VMEM((groups, GROUP * UNIT, hidden), BF16),
                DMA((groups,)),
            ],
            compiler_params=pltpu.CompilerParams(vmem_limit_bytes=50 * 2**20),
            name='score',
        )(table, vmem(q_all), vmem(p_head), vmem(nmt), w_proj, hbm(doc_hidden.reshape(nd * dlen, hidden)))

        scores = pl.pallas_call(
            functools.partial(gather_kernel, nd, tiles),
            out_shape=pltpu.VMEM((nd * 8, nq * 8), F32),
            in_specs=[SMEM, VMEM, VMEM],
            out_specs=VMEM,
            scratch_shapes=[DMA((7,)), DMA((7,))],
            compiler_params=pltpu.CompilerParams(collective_id=1, has_side_effects=True),
            name='gather',
        )(temperature.reshape(1), vmem(best), vmem(seg))

        losses, mean = pl.pallas_call(
            functools.partial(loss_kernel, nq),
            out_shape=[jax.ShapeDtypeStruct((1, nq), F32), jax.ShapeDtypeStruct((1, 1), F32)],
            in_specs=[VMEM],
            out_specs=[VMEM, VMEM],
            name='loss',
        )(vmem(scores))
        return losses.reshape(nq), mean.reshape(1)

    tok, mask, row = P(('replica', 'data2', 'data'), None, None), P(('replica', 'data2', 'data'), None), P(('replica', 'data2', 'data'))
    return jax.shard_map(local_step, mesh=mesh, in_specs=(tok, tok, P(None, None), mask, mask, P()),
                         out_specs=(row, P('replica')), check_vma=False)
```

```python
import functools

import jax
import jax.numpy as jnp
from jax import lax
from jax.experimental import pallas as pl
from jax.experimental.pallas import tpu as pltpu
from jax.sharding import PartitionSpec as P

MESH = pl.DeviceIdType.MESH
F32, BF16 = jnp.float32, jnp.bfloat16
BIG = 1e30
UNIT = 64
LANES = 8
RING = 4
HEAD = 320
GROUP = 16


def iota(shape, dim):
    return lax.broadcasted_iota(jnp.int32, shape, dim)


def dot(a, b):
    return jnp.dot(a, b, preferred_element_type=F32)


def place(rel):
    y, d = lax.axis_index('data2'), lax.axis_index('data')
    x, core = d // 2, d % 2
    y = 1 - y if rel & 4 else y
    x = 1 - x if rel & 2 else x
    core = 1 - core if rel & 1 else core
    return {'data2': y, 'data': x * 2 + core}, y * 4 + x * 2 + core


def unit_rows(projected):
    square = jnp.sum(projected * projected, axis=-1, keepdims=True)
    return (projected * lax.rsqrt(jnp.maximum(square, 1e-24))).astype(BF16)


def mask_features(doc, off):
    return jnp.where(iota(off.shape, 1) == doc, off.astype(F32), 0.0).astype(BF16)


def project_kernel(nq, qlen, nd, dlen, q_hbm, d_hbm, w_hbm, qm_hbm, dm_hbm, q_all, p_ext, table, seg, nmt, w_buf,
                   qm_all, q_buf, dm_buf, d_buf, in_sem, d_sem, qs_sem, qr_sem, ms_sem, mr_sem):
    rows = nq * qlen
    n = nq * 8
    me = place(0)[1]
    as_bf = lambda cond: cond.astype(F32).astype(BF16)
    ins = [pltpu.make_async_copy(src, dst, in_sem.at[k]) for k, (src, dst) in enumerate(
        [(qm_hbm, qm_all.at[pl.ds(me * nq, nq)]), (dm_hbm, dm_buf), (w_hbm, w_buf), (q_hbm, q_buf)])]
    for copy in ins:
        copy.start()

    def doc_copy(j, slot):
        return pltpu.make_async_copy(d_hbm.at[pl.ds(j * dlen, HEAD)], d_buf.at[slot], d_sem.at[slot])

    barrier = pltpu.get_barrier_semaphore()
    for rel in range(1, 8):
        pl.semaphore_signal(barrier, inc=1, device_id=place(rel)[0], device_id_type=MESH)

    def remote(ref, per, origin_rel, to_rel, send_sem, recv_sem):
        block = ref.at[pl.ds(place(origin_rel)[1] * per, per)]
        return pltpu.make_async_remote_copy(src_ref=block, dst_ref=block, send_sem=send_sem, recv_sem=recv_sem,
                                            device_id=place(to_rel)[0], device_id_type=MESH)

    ins[0].wait()
    pl.semaphore_wait(barrier, 7)
    mask_sent = [remote(qm_all, nq, 0, rel, ms_sem.at[rel - 1], mr_sem.at[rel - 1]) for rel in (6, 7, 2, 3, 4, 5, 1)]
    for copy in mask_sent:
        copy.start()

    mask = qm_all[pl.ds(me * nq, nq), :].astype(F32).astype(BF16)
    spread = dot(mask, as_bf(iota((qlen, rows), 1) % qlen == iota((qlen, rows), 0)))
    flat = jnp.sum(jnp.where(iota((nq, rows), 1) // qlen == iota((nq, rows), 0), spread, 0.0), axis=0, keepdims=True)
    before = as_bf(iota((rows, rows), 0) < iota((rows, rows), 1))
    rank = dot(jnp.broadcast_to(flat, (16, rows)).astype(BF16), before)[0:1]
    rank = jnp.where(flat > 0.5, rank, -1.0).astype(jnp.int32)
    pick = as_bf(iota((rows, rows), 0) == rank)

    ins[2].wait()
    ins[3].wait()
    q_vec = unit_rows(dot(q_buf[...], w_buf[...]))
    q_all[pl.ds(me * rows, rows), :] = dot(pick, q_vec).astype(BF16)
    sent = []

    def send(origin_rel, to_rel):
        copy = remote(q_all, rows, origin_rel, to_rel, qs_sem.at[len(sent)], qr_sem.at[(origin_rel ^ to_rel) - 1])
        copy.start()
        sent.append(copy)

    def received(rel):
        remote(q_all, rows, rel, rel, qs_sem.at[0], qr_sem.at[rel - 1]).wait_recv()

    for rel in (2, 4, 6, 1):
        send(0, rel)
    for j in range(RING):
        doc_copy(j, j).start()

    ins[1].wait()
    dmask = dm_buf[...]
    off = jnp.concatenate([1.0 - dmask.astype(F32), jnp.zeros((128 - nd, dlen), F32)], axis=0)
    nmt[...] = jnp.transpose(off).astype(BF16)
    last = jnp.max(dmask * (iota((nd, dlen), 1) + 1), axis=1, keepdims=True).astype(F32)
    count = jnp.floor((last + (UNIT - 1.0)) * (1.0 / UNIT))
    sums = as_bf(iota((nd, nd), 0) >= iota((nd, nd), 1))

    def listing(at, count, per, first):
        upto = dot(sums, jnp.broadcast_to(count, (nd, 128)).astype(BF16))[:, 0:1]
        total = jnp.max(upto, axis=0, keepdims=True)
        slot_id = jnp.minimum(iota((nd, 256), 1).astype(F32), jnp.maximum(total - 1.0, 0.0))
        passed = slot_id >= upto
        unit = slot_id[0:1] + first + jnp.sum(jnp.where(passed, per - count, 0.0), axis=0, keepdims=True)
        doc = jnp.sum(jnp.where(passed, 1.0, 0.0), axis=0, keepdims=True)
        table[at:at + 1, :] = unit.astype(jnp.int32)
        table[at + 1:at + 2, :] = doc.astype(jnp.int32)
        table[at + 2:at + 3, :] = jnp.broadcast_to(total, (1, 256)).astype(jnp.int32)

    head = float(HEAD // UNIT)
    listing(0, jnp.minimum(count, head), head, 0.0)
    listing(4, jnp.maximum(count - head, 0.0), float(dlen // UNIT), head)

    def project(j, carry):
        slot = lax.rem(j, RING)
        doc_copy(j, slot).wait()
        p_ext[pl.ds(j * HEAD, HEAD), 0:128] = unit_rows(dot(d_buf[slot], w_buf[...]))
        p_ext[pl.ds(j * HEAD, HEAD), 128:256] = mask_features(j, nmt[0:HEAD, :])

        @pl.when(j + RING < nd)
        def _():
            doc_copy(j + RING, slot).start()

        return carry

    cut1, cut2 = (8 * nd) // 16, (14 * nd) // 16
    lax.fori_loop(0, cut1, project, 0)
    for rel in (2, 4):
        received(rel)
        send(rel, 1)

    for rel in range(1, 8):
        remote(qm_all, nq, rel, rel, ms_sem.at[rel - 1], mr_sem.at[rel - 1]).wait_recv()
    row, col = iota((n, n), 0), iota((n, n), 1)
    every = qm_all[...].astype(F32).astype(BF16)
    counts = lax.dot_general(jnp.ones((16, qlen), BF16), every, (((1,), (1,)), ((), ())), preferred_element_type=F32)
    counts_bf = counts.astype(BF16)
    in_dev = dot(counts_bf, as_bf((row // nq == col // nq) & (row < col)))
    valid = dot(counts_bf, as_bf(row // nq == col // nq))
    high = jnp.floor(valid * (1.0 / 16.0))
    low = (valid - high * 16.0).astype(BF16)
    high = high.astype(BF16)
    total_of = lambda cond: dot(high, as_bf(cond)) * 16.0 + dot(low, as_bf(cond))
    begin = total_of((row // nq < col // nq) & (row % nq == 0)) + in_dev
    starts = total_of((row // nq < col) & (row % nq == 0))
    table[3:4, 0:128] = starts[0:1].astype(jnp.int32)
    table[3:4, 128:256] = starts[0:1].astype(jnp.int32)
    first = begin[0:1].astype(jnp.int32)
    end = (begin + counts)[0:1].astype(jnp.int32)
    where = iota((rows * 8, n), 0)
    seg[...] = as_bf((where >= first) & (where < end))

    lax.fori_loop(cut1, cut2, project, 0)
    received(6)
    send(6, 1)
    lax.fori_loop(cut2, nd, project, 0)
    for rel in (1, 3, 5, 7):
        received(rel)
    for copy in mask_sent + sent:
        copy.wait_send()


def score_body(nd, rows, tiles, per_doc, hidden, table, q_all, p_head, nmt, w, d_hbm, out, q_list, best, p_tail, d_buf,
               sem, accs):
    n_head, n_tail = table[2, 0], table[6, 0]
    n_group = (n_tail + (GROUP - 1)) // GROUP

    def fetch(g, carry):
        for k in range(GROUP):
            row = pl.multiple_of(table[4, g * GROUP + k] * UNIT, UNIT)
            pltpu.make_async_copy(d_hbm.at[pl.ds(row, UNIT)], d_buf.at[g, pl.ds(k * UNIT, UNIT)],
                                  sem.at[g]).start(priority=k % 2)
        return carry

    lax.fori_loop(0, n_group, fetch, 0)

    floor = jnp.full((nd, 8, 256), -3e38, F32)
    out[...] = jnp.zeros_like(out)
    for dev in range(8):
        q_list[pl.ds(table[3, dev], rows), :] = q_all[dev * rows:(dev + 1) * rows, :].astype(F32)
    q_list[pl.ds(table[3, 7] + rows, 256), :] = jnp.zeros((256, 128), F32)
    n_tile = (table[3, 8] + 255) // 256
    away = jnp.full((256, 128), -BIG, BF16)

    def push(tile):
        q_tile = q_list[pl.ds(pl.multiple_of(tile * 256, 256), 256), :].astype(BF16)
        rhs = jnp.concatenate([q_tile, away], axis=1)
        for unit in range(2):
            pltpu.matmul_push_rhs(rhs, staging_register=0, mxu_index=unit, transpose=True)

    def unstage():
        for unit in range(2):
            pltpu.matmul_acc_lhs(accs[unit][0], jnp.zeros((UNIT, 256), BF16), load_staged_rhs=0)
            pltpu.matmul_pop(accs[unit][0])

    def finish(slot, tile):
        out[tile] = jnp.max(jnp.maximum(best[0][slot], best[1][slot]), axis=1)

    def sweep(at, count, row_of, src, is_last):
        n_trip = (count + (2 * LANES - 1)) // (2 * LANES)
        todo = jnp.where(count > 0, n_tile, 0)

        def drain(unit, k, slot, trip):
            value = pltpu.matmul_pop(accs[unit][k])
            top = value[0:8]
            for r in range(1, UNIT // 8):
                top = jnp.maximum(top, value[8 * r:8 * r + 8])
            doc = table[at + 1, jnp.maximum(trip, 0) * (2 * LANES) + 2 * k + unit]
            best[unit][slot, doc] = jnp.maximum(best[unit][slot, doc], top)

        def step(slot, trip, prev_slot, prev_trip, first):
            for k in range(LANES):
                for unit in range(2):
                    drain(unit, k, prev_slot, prev_trip)
                    row = row_of(trip * (2 * LANES) + 2 * k + unit) * UNIT
                    lhs = src[pl.ds(pl.multiple_of(row, UNIT), UNIT), :]
                    pltpu.matmul_acc_lhs(accs[unit][k], lhs, load_staged_rhs=0 if first and k == 0 else None)

        push(0)

        def per_tile(tile, carry):
            if not is_last:
                best[0][tile + 1] = floor
                best[1][tile + 1] = floor
            step(tile + 1, 0, tile, n_trip - 1, True)
            if is_last:
                finish(tile, jnp.maximum(tile - 1, 0))
            push(jnp.minimum(tile + 1, tiles - 1))

            def per_trip(trip, carry):
                step(tile + 1, trip, tile + 1, trip - 1, False)
                return carry

            lax.fori_loop(1, n_trip, per_trip, 0)
            return carry

        lax.fori_loop(0, todo, per_tile, 0)
        for k in range(LANES):
            for unit in range(2):
                drain(unit, k, todo, n_trip - 1)
        unstage()

    for unit in range(2):
        best[unit][0] = floor
        for k in range(LANES):
            pltpu.matmul_pop(accs[unit][k])
    sweep(0, n_head, lambda i: table[0, i], p_head, False)

    depth = hidden // 256
    blank = jnp.zeros((256, 128), BF16)

    def push_w(k):
        rhs = jnp.concatenate([w[k * 256:(k + 1) * 256, :], blank], axis=1)
        for unit in range(2):
            pltpu.matmul_push_rhs(rhs, staging_register=0, mxu_index=unit, transpose=False)

    push_w(0)

    def project(g, carry):
        pltpu.make_async_copy(d_hbm.at[pl.ds(0, GROUP * UNIT)], d_buf.at[g], sem.at[g]).wait()
        for half in range(2):
            for k in range(depth):
                for q in range(4):
                    for unit in range(2):
                        at = (half * 8 + unit * 4 + q) * UNIT
                        pltpu.matmul_acc_lhs(accs[unit][half * 4 + q],
                                             d_buf[g, at:at + UNIT, k * 256:(k + 1) * 256],
                                             load_staged_rhs=0 if q == 0 else None)
                push_w((k + 1) % depth)
            for q in range(4):
                for unit in range(2):
                    index = g * GROUP + half * 8 + unit * 4 + q
                    value = pltpu.matmul_pop(accs[unit][half * 4 + q])[:, 0:128]
                    dst = pl.ds(pl.multiple_of(index * UNIT, UNIT), UNIT)
                    doc = table[5, index]
                    off = nmt[pl.ds(pl.multiple_of((table[4, index] - doc * per_doc) * UNIT, UNIT), UNIT), :]
                    p_tail[dst, 0:128] = unit_rows(value)
                    p_tail[dst, 128:256] = mask_features(doc, off)
        return carry

    lax.fori_loop(0, n_group, project, 0)
    unstage()

    sweep(4, n_tail, lambda i: jnp.minimum(i, n_tail - 1), p_tail, True)

    def finish_all(tile, carry):
        finish(tile + 1, tile)
        return carry

    lax.fori_loop(jnp.where(n_tail > 0, n_tile - 1, 0), n_tile, finish_all, 0)


def score_kernel(nd, rows, tiles, per_doc, hidden, table, q_all, p_head, nmt, w, d_hbm, out, q_list, best0, best1, p_tail,
                 d_buf, sem):
    def body(*accs):
        score_body(nd, rows, tiles, per_doc, hidden, table, q_all, p_head, nmt, w, d_hbm, out, q_list, (best0, best1),
                   p_tail, d_buf, sem, (accs[:LANES], accs[LANES:]))

    pl.run_scoped(body, *[pltpu.ACC(0)((UNIT, 256), F32)] * LANES, *[pltpu.ACC(1)((UNIT, 256), F32)] * LANES)


def gather_kernel(nd, tiles, temp, best, seg, scores, send_sem, recv_sem):
    me = place(0)[1]
    barrier = pltpu.get_barrier_semaphore()
    for rel in range(1, 8):
        pl.semaphore_signal(barrier, inc=1, device_id=place(rel)[0], device_id_type=MESH)
    total = jnp.zeros((nd, nd * 8), F32)
    for t in range(tiles):
        value = best[t]
        high = value.astype(BF16)
        rest = value - high.astype(F32)
        mid = rest.astype(BF16)
        low = (rest - mid.astype(F32)).astype(BF16)
        part = dot(jnp.concatenate([high, mid, low], axis=0), seg[t * 256:(t + 1) * 256, :])
        total = total + ((part[0:nd] + part[nd:2 * nd]) + part[2 * nd:3 * nd])
    scores[pl.ds(me * nd, nd), :] = total / temp[0]
    pl.semaphore_wait(barrier, 7)

    def remote(origin_rel, rel):
        block = scores.at[pl.ds(place(origin_rel)[1] * nd, nd)]
        return pltpu.make_async_remote_copy(src_ref=block, dst_ref=block, send_sem=send_sem.at[rel - 1],
                                            recv_sem=recv_sem.at[rel - 1], device_id=place(rel)[0], device_id_type=MESH)

    copies = [remote(0, rel) for rel in (6, 7, 2, 3, 4, 5, 1)]
    for copy in copies:
        copy.start()
    for rel in range(1, 8):
        remote(rel, rel).wait_recv()
    for copy in copies:
        copy.wait_send()


def loss_kernel(nq, scores, losses, mean):
    n = nq * 8
    me = place(0)[1]
    logits = scores[...]
    own = jnp.sum(jnp.where(iota((n, n), 0) == iota((n, n), 1), logits, 0.0), axis=0, keepdims=True)
    peak = jnp.max(logits, axis=0, keepdims=True)
    loss = jnp.log(jnp.sum(jnp.exp(logits - peak), axis=0, keepdims=True)) + peak - own
    mean[...] = jnp.sum(loss, axis=1, keepdims=True) / n
    row, col = iota((nq, n), 0), iota((nq, n), 1)
    picked = jnp.sum(jnp.where(col == me * nq + row, loss, 0.0), axis=1, keepdims=True)
    losses[...] = jnp.sum(jnp.where(col == row, picked, 0.0), axis=0, keepdims=True)[:, 0:nq]


VMEM = pl.BlockSpec(memory_space=pltpu.VMEM)
SMEM = pl.BlockSpec(memory_space=pltpu.SMEM)
ANY = pl.BlockSpec(memory_space=pl.ANY)
DMA = pltpu.SemaphoreType.DMA


def solution(mesh):
    def local_step(query_hidden, doc_hidden, w_proj, query_mask, doc_mask, temperature):
        nq, qlen, hidden = query_hidden.shape
        nd, dlen, _ = doc_hidden.shape
        rows = nq * qlen
        tiles = rows * 8 // 256
        hbm = lambda x: pltpu.with_memory_space_constraint(x, pltpu.HBM)
        vmem = lambda x: pltpu.with_memory_space_constraint(x, pltpu.VMEM)
        q_all, p_head, table, seg, nmt, w_vmem = pl.pallas_call(
            functools.partial(project_kernel, nq, qlen, nd, dlen),
            out_shape=[
                pltpu.VMEM((rows * 8, 128), BF16),
                pltpu.VMEM((nd * HEAD, 256), BF16),
                pltpu.VMEM((8, 256), jnp.int32),
                pltpu.VMEM((rows * 8, nq * 8), BF16),
                pltpu.VMEM((dlen, 128), BF16),
                pltpu.VMEM((hidden, 128), BF16),
            ],
            in_specs=[ANY] * 5,
            out_specs=[VMEM] * 6,
            scratch_shapes=[
                pltpu.VMEM((nq * 8, qlen), jnp.int32),
                pltpu.VMEM((rows, hidden), BF16),
                pltpu.VMEM((nd, dlen), jnp.int32),
                pltpu.VMEM((RING, HEAD, hidden), BF16),
                DMA((4,)), DMA((RING,)), DMA((7,)), DMA((7,)), DMA((7,)), DMA((7,)),
            ],
            compiler_params=pltpu.CompilerParams(collective_id=0, has_side_effects=True, vmem_limit_bytes=30 * 2**20),
            name='project',
        )(hbm(query_hidden.reshape(rows, hidden)), hbm(doc_hidden.reshape(nd * dlen, hidden)), hbm(w_proj),
          hbm(query_mask), hbm(doc_mask))

        tail_rows = nd * (dlen - HEAD)
        groups = tail_rows // (GROUP * UNIT)
        best = pl.pallas_call(
            functools.partial(score_kernel, nd, rows, tiles, dlen // UNIT, hidden),
            out_shape=pltpu.VMEM((tiles, nd, 256), F32),
            in_specs=[SMEM, VMEM, VMEM, VMEM, VMEM, ANY],
            out_specs=VMEM,
            scratch_shapes=[
                pltpu.VMEM((rows * 8 + 512, 128), F32),
                pltpu.VMEM((tiles + 1, nd, 8, 256), F32),
                pltpu.VMEM((tiles + 1, nd, 8, 256), F32),
                pltpu.VMEM((tail_rows, 256), BF16),
                pltpu.VMEM((groups, GROUP * UNIT, hidden), BF16),
                DMA((groups,)),
            ],
            compiler_params=pltpu.CompilerParams(vmem_limit_bytes=50 * 2**20),
            name='score',
        )(table, vmem(q_all), vmem(p_head), vmem(nmt), vmem(w_vmem), hbm(doc_hidden.reshape(nd * dlen, hidden)))

        scores = pl.pallas_call(
            functools.partial(gather_kernel, nd, tiles),
            out_shape=pltpu.VMEM((nd * 8, nq * 8), F32),
            in_specs=[SMEM, VMEM, VMEM],
            out_specs=VMEM,
            scratch_shapes=[DMA((7,)), DMA((7,))],
            compiler_params=pltpu.CompilerParams(collective_id=1, has_side_effects=True),
            name='gather',
        )(temperature.reshape(1), vmem(best), vmem(seg))

        losses, mean = pl.pallas_call(
            functools.partial(loss_kernel, nq),
            out_shape=[jax.ShapeDtypeStruct((1, nq), F32), jax.ShapeDtypeStruct((1, 1), F32)],
            in_specs=[VMEM],
            out_specs=[VMEM, VMEM],
            name='loss',
        )(vmem(scores))
        return losses.reshape(nq), mean.reshape(1)

    tok, mask, row = P(('replica', 'data2', 'data'), None, None), P(('replica', 'data2', 'data'), None), P(('replica', 'data2', 'data'))
    return jax.shard_map(local_step, mesh=mesh, in_specs=(tok, tok, P(None, None), mask, mask, P()),
                         out_specs=(row, P('replica')), check_vma=False)
```

```python
import functools

import jax
import jax.numpy as jnp
from jax import lax
from jax.experimental import pallas as pl
from jax.experimental.pallas import tpu as pltpu
from jax.sharding import PartitionSpec as P

MESH = pl.DeviceIdType.MESH
F32, BF16 = jnp.float32, jnp.bfloat16
BIG = 1e30
UNIT = 64
LANES = 8
RING = 4
HEAD = 320
GROUP = 8


def iota(shape, dim):
    return lax.broadcasted_iota(jnp.int32, shape, dim)


def dot(a, b):
    return jnp.dot(a, b, preferred_element_type=F32)


def place(rel):
    y, d = lax.axis_index('data2'), lax.axis_index('data')
    x, core = d // 2, d % 2
    y = 1 - y if rel & 4 else y
    x = 1 - x if rel & 2 else x
    core = 1 - core if rel & 1 else core
    return {'data2': y, 'data': x * 2 + core}, y * 4 + x * 2 + core


def unit_rows(projected):
    square = jnp.sum(projected * projected, axis=-1, keepdims=True)
    return (projected * lax.rsqrt(jnp.maximum(square, 1e-24))).astype(BF16)


def mask_features(doc, off):
    return jnp.where(iota(off.shape, 1) == doc, off.astype(F32), 0.0).astype(BF16)


def project_kernel(nq, qlen, nd, dlen, q_hbm, d_hbm, w_hbm, qm_hbm, dm_hbm, q_all, p_ext, table, seg, nmt, w_buf,
                   qm_all, q_buf, dm_buf, d_buf, in_sem, d_sem, qs_sem, qr_sem, ms_sem, mr_sem):
    rows = nq * qlen
    n = nq * 8
    me = place(0)[1]
    as_bf = lambda cond: cond.astype(F32).astype(BF16)
    ins = [pltpu.make_async_copy(src, dst, in_sem.at[k]) for k, (src, dst) in enumerate(
        [(qm_hbm, qm_all.at[pl.ds(me * nq, nq)]), (dm_hbm, dm_buf), (w_hbm, w_buf), (q_hbm, q_buf)])]
    for copy in ins:
        copy.start()

    def doc_copy(j, slot):
        return pltpu.make_async_copy(d_hbm.at[pl.ds(j * dlen, HEAD)], d_buf.at[slot], d_sem.at[slot])

    for j in range(2):
        doc_copy(j, j).start()
    barrier = pltpu.get_barrier_semaphore()
    for rel in range(1, 8):
        pl.semaphore_signal(barrier, inc=1, device_id=place(rel)[0], device_id_type=MESH)

    def remote(ref, per, origin_rel, to_rel, send_sem, recv_sem):
        block = ref.at[pl.ds(place(origin_rel)[1] * per, per)]
        return pltpu.make_async_remote_copy(src_ref=block, dst_ref=block, send_sem=send_sem, recv_sem=recv_sem,
                                            device_id=place(to_rel)[0], device_id_type=MESH)

    ins[0].wait()
    pl.semaphore_wait(barrier, 7)
    mask_sent = [remote(qm_all, nq, 0, rel, ms_sem.at[rel - 1], mr_sem.at[rel - 1]) for rel in (6, 7, 2, 3, 4, 5, 1)]
    for copy in mask_sent:
        copy.start()

    mask = qm_all[pl.ds(me * nq, nq), :].astype(F32).astype(BF16)
    spread = dot(mask, as_bf(iota((qlen, rows), 1) % qlen == iota((qlen, rows), 0)))
    flat = jnp.sum(jnp.where(iota((nq, rows), 1) // qlen == iota((nq, rows), 0), spread, 0.0), axis=0, keepdims=True)
    before = as_bf(iota((rows, rows), 0) < iota((rows, rows), 1))
    rank = dot(jnp.broadcast_to(flat, (16, rows)).astype(BF16), before)[0:1]
    rank = jnp.where(flat > 0.5, rank, -1.0).astype(jnp.int32)
    pick = as_bf(iota((rows, rows), 0) == rank)

    ins[2].wait()
    ins[3].wait()
    q_vec = unit_rows(dot(q_buf[...], w_buf[...]))
    q_all[pl.ds(me * rows, rows), :] = dot(pick, q_vec).astype(BF16)
    sent = []

    def send(origin_rel, to_rel):
        copy = remote(q_all, rows, origin_rel, to_rel, qs_sem.at[len(sent)], qr_sem.at[(origin_rel ^ to_rel) - 1])
        copy.start()
        sent.append(copy)

    def received(rel):
        remote(q_all, rows, rel, rel, qs_sem.at[0], qr_sem.at[rel - 1]).wait_recv()

    for rel in (2, 4, 6, 1):
        send(0, rel)
    for j in range(2, RING):
        doc_copy(j, j).start()

    ins[1].wait()
    dmask = dm_buf[...]
    off = jnp.concatenate([1.0 - dmask.astype(F32), jnp.zeros((128 - nd, dlen), F32)], axis=0)
    nmt[...] = jnp.transpose(off).astype(BF16)
    last = jnp.max(dmask * (iota((nd, dlen), 1) + 1), axis=1, keepdims=True).astype(F32)
    count = jnp.floor((last + (UNIT - 1.0)) * (1.0 / UNIT))
    sums = as_bf(iota((nd, nd), 0) >= iota((nd, nd), 1))

    def listing(at, count, first):
        upto = dot(sums, jnp.broadcast_to(count, (nd, 128)).astype(BF16))[:, 0:1]
        total = jnp.max(upto, axis=0, keepdims=True)
        slot_id = jnp.minimum(iota((nd, 256), 1).astype(F32), jnp.maximum(total - 1.0, 0.0))
        passed = slot_id >= upto
        unit = slot_id[0:1] + first + jnp.sum(jnp.where(passed, per_doc - count, 0.0), axis=0, keepdims=True)
        doc = jnp.sum(jnp.where(passed, 1.0, 0.0), axis=0, keepdims=True)
        table[at:at + 1, :] = unit.astype(jnp.int32)
        table[at + 1:at + 2, :] = doc.astype(jnp.int32)
        table[at + 2:at + 3, :] = jnp.broadcast_to(total, (1, 256)).astype(jnp.int32)

    head, per_doc = float(HEAD // UNIT), float(dlen // UNIT)
    listing(0, jnp.minimum(count, head), 0.0)
    listing(4, jnp.maximum(count - head, 0.0), head)

    def project(j, carry):
        slot = lax.rem(j, RING)
        doc_copy(j, slot).wait()
        p_ext[pl.ds(j * dlen, HEAD), 0:128] = unit_rows(dot(d_buf[slot], w_buf[...]))
        p_ext[pl.ds(j * dlen, HEAD), 128:256] = mask_features(j, nmt[0:HEAD, :])

        @pl.when(j + RING < nd)
        def _():
            doc_copy(j + RING, slot).start()

        return carry

    cut1, cut2 = (8 * nd) // 16, (14 * nd) // 16
    lax.fori_loop(0, cut1, project, 0)
    for rel in (2, 4):
        received(rel)
        send(rel, 1)

    for rel in range(1, 8):
        remote(qm_all, nq, rel, rel, ms_sem.at[rel - 1], mr_sem.at[rel - 1]).wait_recv()
    row, col = iota((n, n), 0), iota((n, n), 1)
    every = qm_all[...].astype(F32).astype(BF16)
    counts = lax.dot_general(jnp.ones((16, qlen), BF16), every, (((1,), (1,)), ((), ())), preferred_element_type=F32)
    counts_bf = counts.astype(BF16)
    in_dev = dot(counts_bf, as_bf((row // nq == col // nq) & (row < col)))
    valid = dot(counts_bf, as_bf(row // nq == col // nq))
    high = jnp.floor(valid * (1.0 / 16.0))
    low = (valid - high * 16.0).astype(BF16)
    high = high.astype(BF16)
    total_of = lambda cond: dot(high, as_bf(cond)) * 16.0 + dot(low, as_bf(cond))
    begin = total_of((row // nq < col // nq) & (row % nq == 0)) + in_dev
    starts = total_of((row // nq < col) & (row % nq == 0))
    table[3:4, 0:128] = starts[0:1].astype(jnp.int32)
    table[3:4, 128:256] = starts[0:1].astype(jnp.int32)
    first = begin[0:1].astype(jnp.int32)
    end = (begin + counts)[0:1].astype(jnp.int32)
    where = iota((rows * 8, n), 0)
    seg[...] = as_bf((where >= first) & (where < end))

    lax.fori_loop(cut1, cut2, project, 0)
    received(6)
    send(6, 1)
    lax.fori_loop(cut2, nd, project, 0)
    for rel in (1, 3, 5, 7):
        received(rel)
    for copy in mask_sent + sent:
        copy.wait_send()


def score_body(nd, rows, tiles, per_doc, hidden, table, q_all, nmt, w, d_hbm, out, p_ext, q_list, best, d_buf,
               sem, accs):
    n_head, n_tail = table[2, 0], table[6, 0]
    n_group = (n_tail + (GROUP - 1)) // GROUP

    def fetch(g, carry):
        for k in range(GROUP):
            row = pl.multiple_of(table[4, g * GROUP + k] * UNIT, UNIT)
            pltpu.make_async_copy(d_hbm.at[pl.ds(row, UNIT)], d_buf.at[g, pl.ds(k * UNIT, UNIT)],
                                  sem.at[g]).start(priority=k % 2)
        return carry

    lax.fori_loop(0, n_group, fetch, 0)

    floor = jnp.full((nd, 8, 256), -3e38, F32)
    out[...] = jnp.zeros_like(out)
    for dev in range(8):
        q_list[pl.ds(table[3, dev], rows), :] = q_all[dev * rows:(dev + 1) * rows, :].astype(F32)
    q_list[pl.ds(table[3, 7] + rows, 256), :] = jnp.zeros((256, 128), F32)
    n_tile = (table[3, 8] + 255) // 256
    away = jnp.full((256, 128), -BIG, BF16)

    def push(tile):
        q_tile = q_list[pl.ds(pl.multiple_of(tile * 256, 256), 256), :].astype(BF16)
        rhs = jnp.concatenate([q_tile, away], axis=1)
        for unit in range(2):
            pltpu.matmul_push_rhs(rhs, staging_register=0, mxu_index=unit, transpose=True)

    def unstage():
        for unit in range(2):
            pltpu.matmul_acc_lhs(accs[unit][0], jnp.zeros((UNIT, 256), BF16), load_staged_rhs=0)
            pltpu.matmul_pop(accs[unit][0])

    def finish(slot, tile):
        out[tile] = jnp.max(jnp.maximum(best[0][slot], best[1][slot]), axis=1)

    def sweep(count, item, is_last):
        n_trip = (count + (2 * LANES - 1)) // (2 * LANES)
        todo = jnp.where(count > 0, n_tile, 0)

        def drain(unit, k, slot, trip):
            value = pltpu.matmul_pop(accs[unit][k])
            top = value[0:8]
            for r in range(1, UNIT // 8):
                top = jnp.maximum(top, value[8 * r:8 * r + 8])
            doc = item(trip * (2 * LANES) + 2 * k + unit, 1)
            best[unit][slot, doc] = jnp.maximum(best[unit][slot, doc], top)

        def step(slot, trip, prev_slot, prev_trip, first):
            for k in range(LANES):
                for unit in range(2):
                    drain(unit, k, prev_slot, prev_trip)
                    row = item(trip * (2 * LANES) + 2 * k + unit, 0) * UNIT
                    lhs = p_ext[pl.ds(pl.multiple_of(row, UNIT), UNIT), :]
                    pltpu.matmul_acc_lhs(accs[unit][k], lhs, load_staged_rhs=0 if first and k == 0 else None)

        push(0)

        def per_tile(tile, carry):
            if not is_last:
                best[0][tile + 1] = floor
                best[1][tile + 1] = floor
            step(tile + 1, 0, tile, n_trip - 1, True)
            if is_last:
                finish(tile, jnp.maximum(tile - 1, 0))
            push(jnp.minimum(tile + 1, tiles - 1))

            def per_trip(trip, carry):
                step(tile + 1, trip, tile + 1, trip - 1, False)
                return carry

            lax.fori_loop(1, n_trip, per_trip, 0)
            return carry

        lax.fori_loop(0, todo, per_tile, 0)
        for k in range(LANES):
            for unit in range(2):
                drain(unit, k, todo, n_trip - 1)
        unstage()

    for unit in range(2):
        best[unit][0] = floor
        for k in range(LANES):
            pltpu.matmul_pop(accs[unit][k])
    n_first = n_head // (2 * LANES) * (2 * LANES)
    n_left = n_head - n_first
    n_second = n_left + n_tail

    def second(i, what):
        i = jnp.maximum(jnp.minimum(i, n_second - 1), 0)
        return jnp.where(i < n_left, table[what, n_first + i], table[4 + what, jnp.maximum(i - n_left, 0)])

    sweep(n_first, lambda i, what: table[what, jnp.maximum(i, 0)], False)

    depth = hidden // 256
    blank = jnp.zeros((256, 128), BF16)

    def push_w(k):
        rhs = jnp.concatenate([w[k * 256:(k + 1) * 256, :], blank], axis=1)
        for unit in range(2):
            pltpu.matmul_push_rhs(rhs, staging_register=0, mxu_index=unit, transpose=False)

    push_w(0)

    def project(g, carry):
        pltpu.make_async_copy(d_hbm.at[pl.ds(0, GROUP * UNIT)], d_buf.at[g], sem.at[g]).wait()
        for k in range(depth):
            for q in range(4):
                for unit in range(2):
                    at = (unit * 4 + q) * UNIT
                    pltpu.matmul_acc_lhs(accs[unit][q], d_buf[g, at:at + UNIT, k * 256:(k + 1) * 256],
                                         load_staged_rhs=0 if q == 0 else None)
            push_w((k + 1) % depth)
        for q in range(4):
            for unit in range(2):
                block, doc = table[4, g * GROUP + unit * 4 + q], table[5, g * GROUP + unit * 4 + q]
                value = pltpu.matmul_pop(accs[unit][q])[:, 0:128]
                dst = pl.ds(pl.multiple_of(block * UNIT, UNIT), UNIT)
                off = nmt[pl.ds(pl.multiple_of((block - doc * per_doc) * UNIT, UNIT), UNIT), :]
                p_ext[dst, 0:128] = unit_rows(value)
                p_ext[dst, 128:256] = mask_features(doc, off)
        return carry

    lax.fori_loop(0, n_group, project, 0)
    unstage()

    sweep(n_second, second, True)

    def finish_all(tile, carry):
        finish(tile + 1, tile)
        return carry

    lax.fori_loop(jnp.where(n_second > 0, n_tile - 1, 0), n_tile, finish_all, 0)


def score_kernel(nd, rows, tiles, per_doc, hidden, table, q_all, p_in, nmt, w, d_hbm, out, p_ext, q_list, best0, best1,
                 d_buf, sem):
    def body(*accs):
        score_body(nd, rows, tiles, per_doc, hidden, table, q_all, nmt, w, d_hbm, out, p_ext, q_list, (best0, best1),
                   d_buf, sem, (accs[:LANES], accs[LANES:]))

    pl.run_scoped(body, *[pltpu.ACC(0)((UNIT, 256), F32)] * LANES, *[pltpu.ACC(1)((UNIT, 256), F32)] * LANES)


def gather_kernel(nd, tiles, temp, best, seg, scores, send_sem, recv_sem):
    me = place(0)[1]
    barrier = pltpu.get_barrier_semaphore()
    for rel in range(1, 8):
        pl.semaphore_signal(barrier, inc=1, device_id=place(rel)[0], device_id_type=MESH)
    total = jnp.zeros((nd, nd * 8), F32)
    for t in range(tiles):
        value = best[t]
        high = value.astype(BF16)
        rest = value - high.astype(F32)
        mid = rest.astype(BF16)
        low = (rest - mid.astype(F32)).astype(BF16)
        part = dot(jnp.concatenate([high, mid, low], axis=0), seg[t * 256:(t + 1) * 256, :])
        total = total + ((part[0:nd] + part[nd:2 * nd]) + part[2 * nd:3 * nd])
    scores[pl.ds(me * nd, nd), :] = total / temp[0]
    pl.semaphore_wait(barrier, 7)

    def remote(origin_rel, rel):
        block = scores.at[pl.ds(place(origin_rel)[1] * nd, nd)]
        return pltpu.make_async_remote_copy(src_ref=block, dst_ref=block, send_sem=send_sem.at[rel - 1],
                                            recv_sem=recv_sem.at[rel - 1], device_id=place(rel)[0], device_id_type=MESH)

    copies = [remote(0, rel) for rel in (6, 7, 2, 3, 4, 5, 1)]
    for copy in copies:
        copy.start()
    for rel in range(1, 8):
        remote(rel, rel).wait_recv()
    for copy in copies:
        copy.wait_send()


def loss_kernel(nq, scores, losses, mean):
    n = nq * 8
    me = place(0)[1]
    logits = scores[...]
    own = jnp.sum(jnp.where(iota((n, n), 0) == iota((n, n), 1), logits, 0.0), axis=0, keepdims=True)
    peak = jnp.max(logits, axis=0, keepdims=True)
    loss = jnp.log(jnp.sum(jnp.exp(logits - peak), axis=0, keepdims=True)) + peak - own
    mean[...] = jnp.sum(loss, axis=1, keepdims=True) / n
    row, col = iota((nq, n), 0), iota((nq, n), 1)
    picked = jnp.sum(jnp.where(col == me * nq + row, loss, 0.0), axis=1, keepdims=True)
    losses[...] = jnp.sum(jnp.where(col == row, picked, 0.0), axis=0, keepdims=True)[:, 0:nq]


VMEM = pl.BlockSpec(memory_space=pltpu.VMEM)
SMEM = pl.BlockSpec(memory_space=pltpu.SMEM)
ANY = pl.BlockSpec(memory_space=pl.ANY)
DMA = pltpu.SemaphoreType.DMA


def solution(mesh):
    def local_step(query_hidden, doc_hidden, w_proj, query_mask, doc_mask, temperature):
        nq, qlen, hidden = query_hidden.shape
        nd, dlen, _ = doc_hidden.shape
        rows = nq * qlen
        tiles = rows * 8 // 256
        hbm = lambda x: pltpu.with_memory_space_constraint(x, pltpu.HBM)
        vmem = lambda x: pltpu.with_memory_space_constraint(x, pltpu.VMEM)
        q_all, p_head, table, seg, nmt, w_vmem = pl.pallas_call(
            functools.partial(project_kernel, nq, qlen, nd, dlen),
            out_shape=[
                pltpu.VMEM((rows * 8, 128), BF16),
                pltpu.VMEM((nd * dlen, 256), BF16),
                pltpu.VMEM((8, 256), jnp.int32),
                pltpu.VMEM((rows * 8, nq * 8), BF16),
                pltpu.VMEM((dlen, 128), BF16),
                pltpu.VMEM((hidden, 128), BF16),
            ],
            in_specs=[ANY] * 5,
            out_specs=[VMEM] * 6,
            scratch_shapes=[
                pltpu.VMEM((nq * 8, qlen), jnp.int32),
                pltpu.VMEM((rows, hidden), BF16),
                pltpu.VMEM((nd, dlen), jnp.int32),
                pltpu.VMEM((RING, HEAD, hidden), BF16),
                DMA((4,)), DMA((RING,)), DMA((7,)), DMA((7,)), DMA((7,)), DMA((7,)),
            ],
            compiler_params=pltpu.CompilerParams(collective_id=0, has_side_effects=True, vmem_limit_bytes=30 * 2**20),
            name='project',
        )(hbm(query_hidden.reshape(rows, hidden)), hbm(doc_hidden.reshape(nd * dlen, hidden)), hbm(w_proj),
          hbm(query_mask), hbm(doc_mask))

        tail_rows = nd * (dlen - HEAD)
        groups = tail_rows // (GROUP * UNIT)
        best, _ = pl.pallas_call(
            functools.partial(score_kernel, nd, rows, tiles, dlen // UNIT, hidden),
            out_shape=[pltpu.VMEM((tiles, nd, 256), F32), pltpu.VMEM((nd * dlen, 256), BF16)],
            in_specs=[SMEM, VMEM, VMEM, VMEM, VMEM, ANY],
            out_specs=[VMEM, VMEM],
            input_output_aliases={2: 1},
            scratch_shapes=[
                pltpu.VMEM((rows * 8 + 512, 128), F32),
                pltpu.VMEM((tiles + 1, nd, 8, 256), F32),
                pltpu.VMEM((tiles + 1, nd, 8, 256), F32),
                pltpu.VMEM((groups, GROUP * UNIT, hidden), BF16),
                DMA((groups,)),
            ],
            compiler_params=pltpu.CompilerParams(vmem_limit_bytes=36 * 2**20),
            name='score',
        )(table, vmem(q_all), vmem(p_head), vmem(nmt), vmem(w_vmem), hbm(doc_hidden.reshape(nd * dlen, hidden)))

        scores = pl.pallas_call(
            functools.partial(gather_kernel, nd, tiles),
            out_shape=pltpu.VMEM((nd * 8, nq * 8), F32),
            in_specs=[SMEM, VMEM, VMEM],
            out_specs=VMEM,
            scratch_shapes=[DMA((7,)), DMA((7,))],
            compiler_params=pltpu.CompilerParams(collective_id=1, has_side_effects=True),
            name='gather',
        )(temperature.reshape(1), vmem(best), vmem(seg))

        losses, mean = pl.pallas_call(
            functools.partial(loss_kernel, nq),
            out_shape=[jax.ShapeDtypeStruct((1, nq), F32), jax.ShapeDtypeStruct((1, 1), F32)],
            in_specs=[VMEM],
            out_specs=[VMEM, VMEM],
            name='loss',
        )(vmem(scores))
        return losses.reshape(nq), mean.reshape(1)

    tok, mask, row = P(('replica', 'data2', 'data'), None, None), P(('replica', 'data2', 'data'), None), P(('replica', 'data2', 'data'))
    return jax.shard_map(local_step, mesh=mesh, in_specs=(tok, tok, P(None, None), mask, mask, P()),
                         out_specs=(row, P('replica')), check_vma=False)
```

```python
import functools

import jax
import jax.numpy as jnp
from jax import lax
from jax.experimental import pallas as pl
from jax.experimental.pallas import tpu as pltpu
from jax.sharding import PartitionSpec as P

MESH = pl.DeviceIdType.MESH
F32, BF16 = jnp.float32, jnp.bfloat16
BIG = 1e30
UNIT = 64
LANES = 8
RING = 4
HEAD = 320
GROUP = 8


def iota(shape, dim):
    return lax.broadcasted_iota(jnp.int32, shape, dim)


def dot(a, b):
    return jnp.dot(a, b, preferred_element_type=F32)


def place(rel):
    y, d = lax.axis_index('data2'), lax.axis_index('data')
    x, core = d // 2, d % 2
    y = 1 - y if rel & 4 else y
    x = 1 - x if rel & 2 else x
    core = 1 - core if rel & 1 else core
    return {'data2': y, 'data': x * 2 + core}, y * 4 + x * 2 + core


def unit_rows(projected):
    square = jnp.sum(projected * projected, axis=-1, keepdims=True)
    return (projected * lax.rsqrt(jnp.maximum(square, 1e-24))).astype(BF16)


def mask_features(doc, off):
    return jnp.where(iota(off.shape, 1) == doc, off.astype(F32), 0.0).astype(BF16)


def project_kernel(nq, qlen, nd, dlen, q_hbm, d_hbm, w_hbm, qm_hbm, dm_hbm, q_all, p_ext, table, seg, nmt, w_buf,
                   qm_all, q_buf, dm_buf, d_buf, in_sem, d_sem, qs_sem, qr_sem, ms_sem, mr_sem):
    rows = nq * qlen
    n = nq * 8
    me = place(0)[1]
    as_bf = lambda cond: cond.astype(F32).astype(BF16)
    ins = [pltpu.make_async_copy(src, dst, in_sem.at[k]) for k, (src, dst) in enumerate(
        [(qm_hbm, qm_all.at[pl.ds(me * nq, nq)]), (dm_hbm, dm_buf), (w_hbm, w_buf), (q_hbm, q_buf)])]
    for copy in ins:
        copy.start()

    def doc_copy(j, slot):
        return pltpu.make_async_copy(d_hbm.at[pl.ds(j * dlen, HEAD)], d_buf.at[slot], d_sem.at[slot])

    for j in range(2):
        doc_copy(j, j).start()
    barrier = pltpu.get_barrier_semaphore()
    for rel in range(1, 8):
        pl.semaphore_signal(barrier, inc=1, device_id=place(rel)[0], device_id_type=MESH)

    def remote(ref, per, origin_rel, to_rel, send_sem, recv_sem):
        block = ref.at[pl.ds(place(origin_rel)[1] * per, per)]
        return pltpu.make_async_remote_copy(src_ref=block, dst_ref=block, send_sem=send_sem, recv_sem=recv_sem,
                                            device_id=place(to_rel)[0], device_id_type=MESH)

    ins[0].wait()
    pl.semaphore_wait(barrier, 7)
    mask_sent = [remote(qm_all, nq, 0, rel, ms_sem.at[rel - 1], mr_sem.at[rel - 1]) for rel in (6, 7, 2, 3, 4, 5, 1)]
    for copy in mask_sent:
        copy.start()

    mask = qm_all[pl.ds(me * nq, nq), :].astype(F32).astype(BF16)
    spread = dot(mask, as_bf(iota((qlen, rows), 1) % qlen == iota((qlen, rows), 0)))
    flat = jnp.sum(jnp.where(iota((nq, rows), 1) // qlen == iota((nq, rows), 0), spread, 0.0), axis=0, keepdims=True)
    before = as_bf(iota((rows, rows), 0) < iota((rows, rows), 1))
    rank = dot(jnp.broadcast_to(flat, (16, rows)).astype(BF16), before)[0:1]
    rank = jnp.where(flat > 0.5, rank, -1.0).astype(jnp.int32)
    pick = as_bf(iota((rows, rows), 0) == rank)

    ins[2].wait()
    ins[3].wait()
    q_vec = unit_rows(dot(q_buf[...], w_buf[...]))
    q_all[pl.ds(me * rows, rows), :] = dot(pick, q_vec).astype(BF16)
    sent = []

    def send(origin_rel, to_rel):
        copy = remote(q_all, rows, origin_rel, to_rel, qs_sem.at[len(sent)], qr_sem.at[(origin_rel ^ to_rel) - 1])
        copy.start()
        sent.append(copy)

    def received(rel):
        remote(q_all, rows, rel, rel, qs_sem.at[0], qr_sem.at[rel - 1]).wait_recv()

    for rel in (2, 4, 6, 1):
        send(0, rel)
    for j in range(2, RING):
        doc_copy(j, j).start()

    ins[1].wait()
    dmask = dm_buf[...]
    off = jnp.concatenate([1.0 - dmask.astype(F32), jnp.zeros((128 - nd, dlen), F32)], axis=0)
    nmt[...] = jnp.transpose(off).astype(BF16)
    last = jnp.max(dmask * (iota((nd, dlen), 1) + 1), axis=1, keepdims=True).astype(F32)
    count = jnp.floor((last + (UNIT - 1.0)) * (1.0 / UNIT))
    sums = as_bf(iota((nd, nd), 0) >= iota((nd, nd), 1))

    head, per_doc = float(HEAD // UNIT), float(dlen // UNIT)
    lane = iota((nd, 256), 1).astype(F32)

    def listing(count, first):
        upto = dot(sums, jnp.broadcast_to(count, (nd, 128)).astype(BF16))[:, 0:1]
        total = jnp.max(upto, axis=0, keepdims=True)

        def at(index):
            index = jnp.maximum(jnp.minimum(index, total - 1.0), 0.0)
            passed = index >= upto
            unit = index[0:1] + first + jnp.sum(jnp.where(passed, per_doc - count, 0.0), axis=0, keepdims=True)
            return unit, jnp.sum(jnp.where(passed, 1.0, 0.0), axis=0, keepdims=True)

        return total, at

    def write(at, value):
        table[at:at + 1, :] = jnp.broadcast_to(value, (1, 256)).astype(jnp.int32)

    n_head, head_at = listing(jnp.minimum(count, head), 0.0)
    n_tail, tail_at = listing(jnp.maximum(count - head, 0.0), head)
    n_first = jnp.floor(n_head * (1.0 / (2 * LANES))) * (2.0 * LANES)
    n_left = n_head - n_first
    left, rest = head_at(lane + n_first), tail_at(lane - n_left)
    is_left = (lane[0:1] < n_left) | (n_tail < 0.5)
    write(2, n_head)
    write(6, n_tail)
    for k in range(2):
        write(k, head_at(lane)[k])
        write(4 + k, tail_at(lane)[k])
        write(8 + k, jnp.where(is_left, left[k], rest[k]))

    def project(j, carry):
        slot = lax.rem(j, RING)
        doc_copy(j, slot).wait()
        p_ext[pl.ds(j * dlen, HEAD), 0:128] = unit_rows(dot(d_buf[slot], w_buf[...]))
        p_ext[pl.ds(j * dlen, HEAD), 128:256] = mask_features(j, nmt[0:HEAD, :])

        @pl.when(j + RING < nd)
        def _():
            doc_copy(j + RING, slot).start()

        return carry

    cut1, cut2 = (8 * nd) // 16, (14 * nd) // 16
    lax.fori_loop(0, cut1, project, 0)
    for rel in (2, 4):
        received(rel)
        send(rel, 1)

    for rel in range(1, 8):
        remote(qm_all, nq, rel, rel, ms_sem.at[rel - 1], mr_sem.at[rel - 1]).wait_recv()
    row, col = iota((n, n), 0), iota((n, n), 1)
    every = qm_all[...].astype(F32).astype(BF16)
    counts = lax.dot_general(jnp.ones((16, qlen), BF16), every, (((1,), (1,)), ((), ())), preferred_element_type=F32)
    counts_bf = counts.astype(BF16)
    in_dev = dot(counts_bf, as_bf((row // nq == col // nq) & (row < col)))
    valid = dot(counts_bf, as_bf(row // nq == col // nq))
    high = jnp.floor(valid * (1.0 / 16.0))
    low = (valid - high * 16.0).astype(BF16)
    high = high.astype(BF16)
    total_of = lambda cond: dot(high, as_bf(cond)) * 16.0 + dot(low, as_bf(cond))
    begin = total_of((row // nq < col // nq) & (row % nq == 0)) + in_dev
    starts = total_of((row // nq < col) & (row % nq == 0))
    table[3:4, 0:128] = starts[0:1].astype(jnp.int32)
    table[3:4, 128:256] = starts[0:1].astype(jnp.int32)
    first = begin[0:1].astype(jnp.int32)
    end = (begin + counts)[0:1].astype(jnp.int32)
    where = iota((rows * 8, n), 0)
    seg[...] = as_bf((where >= first) & (where < end))

    lax.fori_loop(cut1, cut2, project, 0)
    received(6)
    send(6, 1)
    lax.fori_loop(cut2, nd, project, 0)
    for rel in (1, 3, 5, 7):
        received(rel)
    for copy in mask_sent + sent:
        copy.wait_send()


def score_body(nd, rows, tiles, per_doc, hidden, table, q_all, nmt, w, d_hbm, out, p_ext, q_list, best, d_buf,
               sem, accs):
    n_head, n_tail = table[2, 0], table[6, 0]
    n_group = (n_tail + (GROUP - 1)) // GROUP

    def fetch(g, carry):
        for k in range(GROUP):
            row = pl.multiple_of(table[4, g * GROUP + k] * UNIT, UNIT)
            pltpu.make_async_copy(d_hbm.at[pl.ds(row, UNIT)], d_buf.at[g, pl.ds(k * UNIT, UNIT)],
                                  sem.at[g]).start(priority=k % 2)
        return carry

    lax.fori_loop(0, n_group, fetch, 0)

    floor = jnp.full((nd, 8, 256), -3e38, F32)
    out[...] = jnp.zeros_like(out)
    for dev in range(8):
        q_list[pl.ds(table[3, dev], rows), :] = q_all[dev * rows:(dev + 1) * rows, :].astype(F32)
    q_list[pl.ds(table[3, 7] + rows, 256), :] = jnp.zeros((256, 128), F32)
    n_tile = (table[3, 8] + 255) // 256
    away = jnp.full((256, 128), -BIG, BF16)

    def push(tile):
        q_tile = q_list[pl.ds(pl.multiple_of(tile * 256, 256), 256), :].astype(BF16)
        rhs = jnp.concatenate([q_tile, away], axis=1)
        for unit in range(2):
            pltpu.matmul_push_rhs(rhs, staging_register=0, mxu_index=unit, transpose=True)

    def unstage():
        for unit in range(2):
            pltpu.matmul_acc_lhs(accs[unit][0], jnp.zeros((UNIT, 256), BF16), load_staged_rhs=0)
            pltpu.matmul_pop(accs[unit][0])

    def finish(slot, tile):
        out[tile] = jnp.max(jnp.maximum(best[0][slot], best[1][slot]), axis=1)

    def sweep(count, at, is_last):
        n_trip = (count + (2 * LANES - 1)) // (2 * LANES)
        todo = jnp.where(count > 0, n_tile, 0)

        def drain(unit, k, slot, trip):
            value = pltpu.matmul_pop(accs[unit][k])
            top = value[0:8]
            for r in range(1, UNIT // 8):
                top = jnp.maximum(top, value[8 * r:8 * r + 8])
            doc = table[at + 1, trip * (2 * LANES) + 2 * k + unit]
            best[unit][slot, doc] = jnp.maximum(best[unit][slot, doc], top)

        def step(slot, trip, prev_slot, prev_trip, first):
            for k in range(LANES):
                for unit in range(2):
                    drain(unit, k, prev_slot, prev_trip)
                    row = table[at, trip * (2 * LANES) + 2 * k + unit] * UNIT
                    lhs = p_ext[pl.ds(pl.multiple_of(row, UNIT), UNIT), :]
                    pltpu.matmul_acc_lhs(accs[unit][k], lhs, load_staged_rhs=0 if first and k == 0 else None)

        push(0)

        def per_tile(tile, carry):
            if not is_last:
                best[0][tile + 1] = floor
                best[1][tile + 1] = floor
            step(tile + 1, 0, tile, n_trip - 1, True)
            if is_last:
                finish(tile, jnp.maximum(tile - 1, 0))
            push(jnp.minimum(tile + 1, tiles - 1))

            def per_trip(trip, carry):
                step(tile + 1, trip, tile + 1, trip - 1, False)
                return carry

            lax.fori_loop(1, n_trip, per_trip, 0)
            return carry

        lax.fori_loop(0, todo, per_tile, 0)
        for k in range(LANES):
            for unit in range(2):
                drain(unit, k, todo, jnp.maximum(n_trip - 1, 0))
        unstage()

    for unit in range(2):
        best[unit][0] = floor
        for k in range(LANES):
            pltpu.matmul_pop(accs[unit][k])
    n_first = n_head // (2 * LANES) * (2 * LANES)
    n_left = n_head - n_first
    n_second = n_left + n_tail

    sweep(n_first, 0, False)

    depth = hidden // 256
    blank = jnp.zeros((256, 128), BF16)

    def push_w(k):
        rhs = jnp.concatenate([w[k * 256:(k + 1) * 256, :], blank], axis=1)
        for unit in range(2):
            pltpu.matmul_push_rhs(rhs, staging_register=0, mxu_index=unit, transpose=False)

    push_w(0)

    def project(g, carry):
        pltpu.make_async_copy(d_hbm.at[pl.ds(0, GROUP * UNIT)], d_buf.at[g], sem.at[g]).wait()
        for k in range(depth):
            for q in range(4):
                for unit in range(2):
                    at = (unit * 4 + q) * UNIT
                    pltpu.matmul_acc_lhs(accs[unit][q], d_buf[g, at:at + UNIT, k * 256:(k + 1) * 256],
                                         load_staged_rhs=0 if q == 0 else None)
            push_w((k + 1) % depth)
        for q in range(4):
            for unit in range(2):
                block, doc = table[4, g * GROUP + unit * 4 + q], table[5, g * GROUP + unit * 4 + q]
                value = pltpu.matmul_pop(accs[unit][q])[:, 0:128]
                dst = pl.ds(pl.multiple_of(block * UNIT, UNIT), UNIT)
                off = nmt[pl.ds(pl.multiple_of((block - doc * per_doc) * UNIT, UNIT), UNIT), :]
                p_ext[dst, 0:128] = unit_rows(value)
                p_ext[dst, 128:256] = mask_features(doc, off)
        return carry

    lax.fori_loop(0, n_group, project, 0)
    unstage()

    sweep(n_second, 8, True)

    def finish_all(tile, carry):
        finish(tile + 1, tile)
        return carry

    lax.fori_loop(jnp.where(n_second > 0, n_tile - 1, 0), n_tile, finish_all, 0)


def score_kernel(nd, rows, tiles, per_doc, hidden, table, q_all, p_in, nmt, w, d_hbm, out, p_ext, q_list, best0, best1,
                 d_buf, sem):
    def body(*accs):
        score_body(nd, rows, tiles, per_doc, hidden, table, q_all, nmt, w, d_hbm, out, p_ext, q_list, (best0, best1),
                   d_buf, sem, (accs[:LANES], accs[LANES:]))

    pl.run_scoped(body, *[pltpu.ACC(0)((UNIT, 256), F32)] * LANES, *[pltpu.ACC(1)((UNIT, 256), F32)] * LANES)


def gather_kernel(nd, tiles, temp, best, seg, scores, send_sem, recv_sem):
    me = place(0)[1]
    barrier = pltpu.get_barrier_semaphore()
    for rel in range(1, 8):
        pl.semaphore_signal(barrier, inc=1, device_id=place(rel)[0], device_id_type=MESH)
    total = jnp.zeros((nd, nd * 8), F32)
    for t in range(tiles):
        value = best[t]
        high = value.astype(BF16)
        rest = value - high.astype(F32)
        mid = rest.astype(BF16)
        low = (rest - mid.astype(F32)).astype(BF16)
        part = dot(jnp.concatenate([high, mid, low], axis=0), seg[t * 256:(t + 1) * 256, :])
        total = total + ((part[0:nd] + part[nd:2 * nd]) + part[2 * nd:3 * nd])
    scores[pl.ds(me * nd, nd), :] = total / temp[0]
    pl.semaphore_wait(barrier, 7)

    def remote(origin_rel, rel):
        block = scores.at[pl.ds(place(origin_rel)[1] * nd, nd)]
        return pltpu.make_async_remote_copy(src_ref=block, dst_ref=block, send_sem=send_sem.at[rel - 1],
                                            recv_sem=recv_sem.at[rel - 1], device_id=place(rel)[0], device_id_type=MESH)

    copies = [remote(0, rel) for rel in (6, 7, 2, 3, 4, 5, 1)]
    for copy in copies:
        copy.start()
    for rel in range(1, 8):
        remote(rel, rel).wait_recv()
    for copy in copies:
        copy.wait_send()


def loss_kernel(nq, scores, losses, mean):
    n = nq * 8
    me = place(0)[1]
    logits = scores[...]
    own = jnp.sum(jnp.where(iota((n, n), 0) == iota((n, n), 1), logits, 0.0), axis=0, keepdims=True)
    peak = jnp.max(logits, axis=0, keepdims=True)
    loss = jnp.log(jnp.sum(jnp.exp(logits - peak), axis=0, keepdims=True)) + peak - own
    mean[...] = jnp.sum(loss, axis=1, keepdims=True) / n
    row, col = iota((nq, n), 0), iota((nq, n), 1)
    picked = jnp.sum(jnp.where(col == me * nq + row, loss, 0.0), axis=1, keepdims=True)
    losses[...] = jnp.sum(jnp.where(col == row, picked, 0.0), axis=0, keepdims=True)[:, 0:nq]


VMEM = pl.BlockSpec(memory_space=pltpu.VMEM)
SMEM = pl.BlockSpec(memory_space=pltpu.SMEM)
ANY = pl.BlockSpec(memory_space=pl.ANY)
DMA = pltpu.SemaphoreType.DMA


def solution(mesh):
    def local_step(query_hidden, doc_hidden, w_proj, query_mask, doc_mask, temperature):
        nq, qlen, hidden = query_hidden.shape
        nd, dlen, _ = doc_hidden.shape
        rows = nq * qlen
        tiles = rows * 8 // 256
        hbm = lambda x: pltpu.with_memory_space_constraint(x, pltpu.HBM)
        vmem = lambda x: pltpu.with_memory_space_constraint(x, pltpu.VMEM)
        q_all, p_head, table, seg, nmt, w_vmem = pl.pallas_call(
            functools.partial(project_kernel, nq, qlen, nd, dlen),
            out_shape=[
                pltpu.VMEM((rows * 8, 128), BF16),
                pltpu.VMEM((nd * dlen, 256), BF16),
                pltpu.VMEM((16, 256), jnp.int32),
                pltpu.VMEM((rows * 8, nq * 8), BF16),
                pltpu.VMEM((dlen, 128), BF16),
                pltpu.VMEM((hidden, 128), BF16),
            ],
            in_specs=[ANY] * 5,
            out_specs=[VMEM] * 6,
            scratch_shapes=[
                pltpu.VMEM((nq * 8, qlen), jnp.int32),
                pltpu.VMEM((rows, hidden), BF16),
                pltpu.VMEM((nd, dlen), jnp.int32),
                pltpu.VMEM((RING, HEAD, hidden), BF16),
                DMA((4,)), DMA((RING,)), DMA((7,)), DMA((7,)), DMA((7,)), DMA((7,)),
            ],
            compiler_params=pltpu.CompilerParams(collective_id=0, has_side_effects=True, vmem_limit_bytes=30 * 2**20),
            name='project',
        )(hbm(query_hidden.reshape(rows, hidden)), hbm(doc_hidden.reshape(nd * dlen, hidden)), hbm(w_proj),
          hbm(query_mask), hbm(doc_mask))

        tail_rows = nd * (dlen - HEAD)
        groups = tail_rows // (GROUP * UNIT)
        best, _ = pl.pallas_call(
            functools.partial(score_kernel, nd, rows, tiles, dlen // UNIT, hidden),
            out_shape=[pltpu.VMEM((tiles, nd, 256), F32), pltpu.VMEM((nd * dlen, 256), BF16)],
            in_specs=[SMEM, VMEM, VMEM, VMEM, VMEM, ANY],
            out_specs=[VMEM, VMEM],
            input_output_aliases={2: 1},
            scratch_shapes=[
                pltpu.VMEM((rows * 8 + 512, 128), F32),
                pltpu.VMEM((tiles + 1, nd, 8, 256), F32),
                pltpu.VMEM((tiles + 1, nd, 8, 256), F32),
                pltpu.VMEM((groups, GROUP * UNIT, hidden), BF16),
                DMA((groups,)),
            ],
            compiler_params=pltpu.CompilerParams(vmem_limit_bytes=36 * 2**20),
            name='score',
        )(table, vmem(q_all), vmem(p_head), vmem(nmt), vmem(w_vmem), hbm(doc_hidden.reshape(nd * dlen, hidden)))

        scores = pl.pallas_call(
            functools.partial(gather_kernel, nd, tiles),
            out_shape=pltpu.VMEM((nd * 8, nq * 8), F32),
            in_specs=[SMEM, VMEM, VMEM],
            out_specs=VMEM,
            scratch_shapes=[DMA((7,)), DMA((7,))],
            compiler_params=pltpu.CompilerParams(collective_id=1, has_side_effects=True),
            name='gather',
        )(temperature.reshape(1), vmem(best), vmem(seg))

        losses, mean = pl.pallas_call(
            functools.partial(loss_kernel, nq),
            out_shape=[jax.ShapeDtypeStruct((1, nq), F32), jax.ShapeDtypeStruct((1, 1), F32)],
            in_specs=[VMEM],
            out_specs=[VMEM, VMEM],
            name='loss',
        )(vmem(scores))
        return losses.reshape(nq), mean.reshape(1)

    tok, mask, row = P(('replica', 'data2', 'data'), None, None), P(('replica', 'data2', 'data'), None), P(('replica', 'data2', 'data'))
    return jax.shard_map(local_step, mesh=mesh, in_specs=(tok, tok, P(None, None), mask, mask, P()),
                         out_specs=(row, P('replica')), check_vma=False)
```

```python
import functools

import jax
import jax.numpy as jnp
from jax import lax
from jax.experimental import pallas as pl
from jax.experimental.pallas import tpu as pltpu
from jax.sharding import PartitionSpec as P

MESH = pl.DeviceIdType.MESH
F32, BF16 = jnp.float32, jnp.bfloat16
BIG = 1e30
UNIT = 64
LANES = 8
RING = 4
HEAD = 320
GROUP = 8


def iota(shape, dim):
    return lax.broadcasted_iota(jnp.int32, shape, dim)


def dot(a, b):
    return jnp.dot(a, b, preferred_element_type=F32)


def place(rel):
    y, d = lax.axis_index('data2'), lax.axis_index('data')
    x, core = d // 2, d % 2
    y = 1 - y if rel & 4 else y
    x = 1 - x if rel & 2 else x
    core = 1 - core if rel & 1 else core
    return {'data2': y, 'data': x * 2 + core}, y * 4 + x * 2 + core


def unit_rows(projected):
    square = jnp.sum(projected * projected, axis=-1, keepdims=True)
    return (projected * lax.rsqrt(jnp.maximum(square, 1e-24))).astype(BF16)


def mask_features(doc, off):
    return jnp.where(iota(off.shape, 1) == doc, off.astype(F32), 0.0).astype(BF16)


def project_kernel(nq, qlen, nd, dlen, q_hbm, d_hbm, w_hbm, qm_hbm, dm_hbm, q_all, p_ext, table, seg, nmt, w_buf,
                   qm_all, q_buf, dm_buf, d_buf, in_sem, d_sem, qs_sem, qr_sem, ms_sem, mr_sem):
    rows = nq * qlen
    n = nq * 8
    me = place(0)[1]
    as_bf = lambda cond: cond.astype(F32).astype(BF16)
    ins = [pltpu.make_async_copy(src, dst, in_sem.at[k]) for k, (src, dst) in enumerate(
        [(qm_hbm, qm_all.at[pl.ds(me * nq, nq)]), (dm_hbm, dm_buf), (w_hbm, w_buf), (q_hbm, q_buf)])]
    for copy in ins:
        copy.start()

    def doc_copy(j, slot):
        return pltpu.make_async_copy(d_hbm.at[pl.ds(j * dlen, HEAD)], d_buf.at[slot], d_sem.at[slot])

    for j in range(RING):
        doc_copy(j, j).start()
    barrier = pltpu.get_barrier_semaphore()
    for rel in range(1, 8):
        pl.semaphore_signal(barrier, inc=1, device_id=place(rel)[0], device_id_type=MESH)

    def remote(ref, per, origin_rel, to_rel, send_sem, recv_sem):
        block = ref.at[pl.ds(place(origin_rel)[1] * per, per)]
        return pltpu.make_async_remote_copy(src_ref=block, dst_ref=block, send_sem=send_sem, recv_sem=recv_sem,
                                            device_id=place(to_rel)[0], device_id_type=MESH)

    ins[0].wait()
    pl.semaphore_wait(barrier, 7)
    mask_sent = [remote(qm_all, nq, 0, rel, ms_sem.at[rel - 1], mr_sem.at[rel - 1]) for rel in (6, 7, 2, 3, 4, 5, 1)]
    for copy in mask_sent:
        copy.start()

    mask = qm_all[pl.ds(me * nq, nq), :].astype(F32).astype(BF16)
    spread = dot(mask, as_bf(iota((qlen, rows), 1) % qlen == iota((qlen, rows), 0)))
    flat = jnp.sum(jnp.where(iota((nq, rows), 1) // qlen == iota((nq, rows), 0), spread, 0.0), axis=0, keepdims=True)
    before = as_bf(iota((rows, rows), 0) < iota((rows, rows), 1))
    rank = dot(jnp.broadcast_to(flat, (16, rows)).astype(BF16), before)[0:1]
    rank = jnp.where(flat > 0.5, rank, -1.0).astype(jnp.int32)
    pick = as_bf(iota((rows, rows), 0) == rank)

    ins[2].wait()
    ins[3].wait()
    q_vec = unit_rows(dot(q_buf[...], w_buf[...]))
    q_all[pl.ds(me * rows, rows), :] = dot(pick, q_vec).astype(BF16)
    sent = []

    def send(origin_rel, to_rel):
        copy = remote(q_all, rows, origin_rel, to_rel, qs_sem.at[len(sent)], qr_sem.at[(origin_rel ^ to_rel) - 1])
        copy.start()
        sent.append(copy)

    def received(rel):
        remote(q_all, rows, rel, rel, qs_sem.at[0], qr_sem.at[rel - 1]).wait_recv()

    for rel in (2, 4, 6, 1):
        send(0, rel)

    ins[1].wait()
    dmask = dm_buf[...]
    off = jnp.concatenate([1.0 - dmask.astype(F32), jnp.zeros((128 - nd, dlen), F32)], axis=0)
    nmt[...] = jnp.transpose(off).astype(BF16)
    last = jnp.max(dmask * (iota((nd, dlen), 1) + 1), axis=1, keepdims=True).astype(F32)
    count = jnp.floor((last + (UNIT - 1.0)) * (1.0 / UNIT))
    sums = as_bf(iota((nd, nd), 0) >= iota((nd, nd), 1))

    head, per_doc = float(HEAD // UNIT), float(dlen // UNIT)
    lane = iota((nd, 256), 1).astype(F32)

    def listing(count, first):
        upto = dot(sums, jnp.broadcast_to(count, (nd, 128)).astype(BF16))[:, 0:1]
        total = jnp.max(upto, axis=0, keepdims=True)

        def at(index):
            index = jnp.maximum(jnp.minimum(index, total - 1.0), 0.0)
            passed = index >= upto
            unit = index[0:1] + first + jnp.sum(jnp.where(passed, per_doc - count, 0.0), axis=0, keepdims=True)
            return unit, jnp.sum(jnp.where(passed, 1.0, 0.0), axis=0, keepdims=True)

        return total, at

    def write(at, value):
        table[at:at + 1, :] = jnp.broadcast_to(value, (1, 256)).astype(jnp.int32)

    n_head, head_at = listing(jnp.minimum(count, head), 0.0)
    n_tail, tail_at = listing(jnp.maximum(count - head, 0.0), head)
    n_first = jnp.floor(n_head * (1.0 / (2 * LANES))) * (2.0 * LANES)
    n_left = n_head - n_first
    left, rest = head_at(lane + n_first), tail_at(lane - n_left)
    is_left = (lane[0:1] < n_left) | (n_tail < 0.5)
    write(2, n_head)
    write(6, n_tail)
    for k in range(2):
        write(k, head_at(lane)[k])
        write(4 + k, tail_at(lane)[k])
        write(8 + k, jnp.where(is_left, left[k], rest[k]))

    def project(j, carry):
        slot = lax.rem(j, RING)
        doc_copy(j, slot).wait()
        p_ext[pl.ds(j * dlen, HEAD), 0:128] = unit_rows(dot(d_buf[slot], w_buf[...]))
        p_ext[pl.ds(j * dlen, HEAD), 128:256] = mask_features(j, nmt[0:HEAD, :])

        @pl.when(j + RING < nd)
        def _():
            doc_copy(j + RING, slot).start()

        return carry

    cut = (11 * nd) // 16
    lax.fori_loop(0, cut, project, 0)
    for rel in (2, 4):
        received(rel)
        send(rel, 1)

    for rel in range(1, 8):
        remote(qm_all, nq, rel, rel, ms_sem.at[rel - 1], mr_sem.at[rel - 1]).wait_recv()
    row, col = iota((n, n), 0), iota((n, n), 1)
    every = qm_all[...].astype(F32).astype(BF16)
    counts = lax.dot_general(jnp.ones((16, qlen), BF16), every, (((1,), (1,)), ((), ())), preferred_element_type=F32)
    counts_bf = counts.astype(BF16)
    in_dev = dot(counts_bf, as_bf((row // nq == col // nq) & (row < col)))
    valid = dot(counts_bf, as_bf(row // nq == col // nq))
    high = jnp.floor(valid * (1.0 / 16.0))
    low = (valid - high * 16.0).astype(BF16)
    high = high.astype(BF16)
    total_of = lambda cond: dot(high, as_bf(cond)) * 16.0 + dot(low, as_bf(cond))
    begin = total_of((row // nq < col // nq) & (row % nq == 0)) + in_dev
    starts = total_of((row // nq < col) & (row % nq == 0))
    table[3:4, 0:128] = starts[0:1].astype(jnp.int32)
    table[3:4, 128:256] = starts[0:1].astype(jnp.int32)
    first = begin[0:1].astype(jnp.int32)
    end = (begin + counts)[0:1].astype(jnp.int32)
    where = iota((rows * 8, n), 0)
    seg[...] = as_bf((where >= first) & (where < end))

    lax.fori_loop(cut, nd, project, 0)
    received(6)
    send(6, 1)
    for rel in (1, 3, 5, 7):
        received(rel)
    for copy in mask_sent + sent:
        copy.wait_send()


def score_body(nd, rows, tiles, per_doc, hidden, table, q_all, nmt, w, d_hbm, out, p_ext, q_list, best, d_buf,
               sem, accs):
    n_head, n_tail = table[2, 0], table[6, 0]
    n_group = (n_tail + (GROUP - 1)) // GROUP

    def fetch(g, carry):
        for k in range(GROUP):
            row = pl.multiple_of(table[4, g * GROUP + k] * UNIT, UNIT)
            pltpu.make_async_copy(d_hbm.at[pl.ds(row, UNIT)], d_buf.at[g, pl.ds(k * UNIT, UNIT)],
                                  sem.at[g]).start(priority=k % 2)
        return carry

    lax.fori_loop(0, n_group, fetch, 0)

    floor = jnp.full((nd, 8, 256), -3e38, F32)
    out[...] = jnp.zeros_like(out)
    for dev in range(8):
        q_list[pl.ds(table[3, dev], rows), :] = q_all[dev * rows:(dev + 1) * rows, :].astype(F32)
    q_list[pl.ds(table[3, 7] + rows, 256), :] = jnp.zeros((256, 128), F32)
    n_tile = (table[3, 8] + 255) // 256
    away = jnp.full((256, 128), -BIG, BF16)

    def push(tile):
        q_tile = q_list[pl.ds(pl.multiple_of(tile * 256, 256), 256), :].astype(BF16)
        rhs = jnp.concatenate([q_tile, away], axis=1)
        for unit in range(2):
            pltpu.matmul_push_rhs(rhs, staging_register=0, mxu_index=unit, transpose=True)

    def unstage():
        for unit in range(2):
            pltpu.matmul_acc_lhs(accs[unit][0], jnp.zeros((UNIT, 256), BF16), load_staged_rhs=0)
            pltpu.matmul_pop(accs[unit][0])

    def finish(slot, tile):
        out[tile] = jnp.max(jnp.maximum(best[0][slot], best[1][slot]), axis=1)

    def sweep(count, at, is_last):
        n_trip = (count + (2 * LANES - 1)) // (2 * LANES)
        todo = jnp.where(count > 0, n_tile, 0)

        def drain(unit, k, slot, trip):
            value = pltpu.matmul_pop(accs[unit][k])
            top = value[0:8]
            for r in range(1, UNIT // 8):
                top = jnp.maximum(top, value[8 * r:8 * r + 8])
            doc = table[at + 1, trip * (2 * LANES) + 2 * k + unit]
            best[unit][slot, doc] = jnp.maximum(best[unit][slot, doc], top)

        def step(slot, trip, prev_slot, prev_trip, first):
            for k in range(LANES):
                for unit in range(2):
                    drain(unit, k, prev_slot, prev_trip)
                    row = table[at, trip * (2 * LANES) + 2 * k + unit] * UNIT
                    lhs = p_ext[pl.ds(pl.multiple_of(row, UNIT), UNIT), :]
                    pltpu.matmul_acc_lhs(accs[unit][k], lhs, load_staged_rhs=0 if first and k == 0 else None)

        push(0)

        def per_tile(tile, carry):
            if not is_last:
                best[0][tile + 1] = floor
                best[1][tile + 1] = floor
            step(tile + 1, 0, tile, n_trip - 1, True)
            if is_last:
                finish(tile, jnp.maximum(tile - 1, 0))
            push(jnp.minimum(tile + 1, tiles - 1))

            def per_trip(trip, carry):
                step(tile + 1, trip, tile + 1, trip - 1, False)
                return carry

            lax.fori_loop(1, n_trip, per_trip, 0)
            return carry

        lax.fori_loop(0, todo, per_tile, 0)
        for k in range(LANES):
            for unit in range(2):
                drain(unit, k, todo, jnp.maximum(n_trip - 1, 0))
        unstage()

    for unit in range(2):
        best[unit][0] = floor
        for k in range(LANES):
            pltpu.matmul_pop(accs[unit][k])
    n_first = n_head // (2 * LANES) * (2 * LANES)
    n_left = n_head - n_first
    n_second = n_left + n_tail

    sweep(n_first, 0, False)

    depth = hidden // 256
    blank = jnp.zeros((256, 128), BF16)

    def push_w(k):
        rhs = jnp.concatenate([w[k * 256:(k + 1) * 256, :], blank], axis=1)
        for unit in range(2):
            pltpu.matmul_push_rhs(rhs, staging_register=0, mxu_index=unit, transpose=False)

    push_w(0)

    def project(g, carry):
        pltpu.make_async_copy(d_hbm.at[pl.ds(0, GROUP * UNIT)], d_buf.at[g], sem.at[g]).wait()
        for k in range(depth):
            for q in range(4):
                for unit in range(2):
                    at = (unit * 4 + q) * UNIT
                    pltpu.matmul_acc_lhs(accs[unit][q], d_buf[g, at:at + UNIT, k * 256:(k + 1) * 256],
                                         load_staged_rhs=0 if q == 0 else None)
            push_w((k + 1) % depth)
        for q in range(4):
            for unit in range(2):
                block, doc = table[4, g * GROUP + unit * 4 + q], table[5, g * GROUP + unit * 4 + q]
                value = pltpu.matmul_pop(accs[unit][q])[:, 0:128]
                dst = pl.ds(pl.multiple_of(block * UNIT, UNIT), UNIT)
                off = nmt[pl.ds(pl.multiple_of((block - doc * per_doc) * UNIT, UNIT), UNIT), :]
                p_ext[dst, 0:128] = unit_rows(value)
                p_ext[dst, 128:256] = mask_features(doc, off)
        return carry

    lax.fori_loop(0, n_group, project, 0)
    unstage()

    sweep(n_second, 8, True)

    def finish_all(tile, carry):
        finish(tile + 1, tile)
        return carry

    lax.fori_loop(jnp.where(n_second > 0, n_tile - 1, 0), n_tile, finish_all, 0)


def score_kernel(nd, rows, tiles, per_doc, hidden, table, q_all, p_in, nmt, w, d_hbm, out, p_ext, q_list, best0, best1,
                 d_buf, sem):
    def body(*accs):
        score_body(nd, rows, tiles, per_doc, hidden, table, q_all, nmt, w, d_hbm, out, p_ext, q_list, (best0, best1),
                   d_buf, sem, (accs[:LANES], accs[LANES:]))

    pl.run_scoped(body, *[pltpu.ACC(0)((UNIT, 256), F32)] * LANES, *[pltpu.ACC(1)((UNIT, 256), F32)] * LANES)


def gather_kernel(nd, tiles, temp, best, seg, scores, send_sem, recv_sem):
    me = place(0)[1]
    barrier = pltpu.get_barrier_semaphore()
    for rel in range(1, 8):
        pl.semaphore_signal(barrier, inc=1, device_id=place(rel)[0], device_id_type=MESH)
    total = jnp.zeros((nd, nd * 8), F32)
    for t in range(tiles):
        value = best[t]
        high = value.astype(BF16)
        rest = value - high.astype(F32)
        mid = rest.astype(BF16)
        low = (rest - mid.astype(F32)).astype(BF16)
        part = dot(jnp.concatenate([high, mid, low], axis=0), seg[t * 256:(t + 1) * 256, :])
        total = total + ((part[0:nd] + part[nd:2 * nd]) + part[2 * nd:3 * nd])
    scores[pl.ds(me * nd, nd), :] = total / temp[0]
    pl.semaphore_wait(barrier, 7)

    def remote(origin_rel, rel):
        block = scores.at[pl.ds(place(origin_rel)[1] * nd, nd)]
        return pltpu.make_async_remote_copy(src_ref=block, dst_ref=block, send_sem=send_sem.at[rel - 1],
                                            recv_sem=recv_sem.at[rel - 1], device_id=place(rel)[0], device_id_type=MESH)

    copies = [remote(0, rel) for rel in (6, 7, 2, 3, 4, 5, 1)]
    for copy in copies:
        copy.start()
    for rel in range(1, 8):
        remote(rel, rel).wait_recv()
    for copy in copies:
        copy.wait_send()


def loss_kernel(nq, scores, losses, mean):
    n = nq * 8
    me = place(0)[1]
    logits = scores[...]
    own = jnp.sum(jnp.where(iota((n, n), 0) == iota((n, n), 1), logits, 0.0), axis=0, keepdims=True)
    peak = jnp.max(logits, axis=0, keepdims=True)
    loss = jnp.log(jnp.sum(jnp.exp(logits - peak), axis=0, keepdims=True)) + peak - own
    mean[...] = jnp.sum(loss, axis=1, keepdims=True) / n
    row, col = iota((nq, n), 0), iota((nq, n), 1)
    picked = jnp.sum(jnp.where(col == me * nq + row, loss, 0.0), axis=1, keepdims=True)
    losses[...] = jnp.sum(jnp.where(col == row, picked, 0.0), axis=0, keepdims=True)[:, 0:nq]


VMEM = pl.BlockSpec(memory_space=pltpu.VMEM)
SMEM = pl.BlockSpec(memory_space=pltpu.SMEM)
ANY = pl.BlockSpec(memory_space=pl.ANY)
DMA = pltpu.SemaphoreType.DMA


def solution(mesh):
    def local_step(query_hidden, doc_hidden, w_proj, query_mask, doc_mask, temperature):
        nq, qlen, hidden = query_hidden.shape
        nd, dlen, _ = doc_hidden.shape
        rows = nq * qlen
        tiles = rows * 8 // 256
        hbm = lambda x: pltpu.with_memory_space_constraint(x, pltpu.HBM)
        vmem = lambda x: pltpu.with_memory_space_constraint(x, pltpu.VMEM)
        q_all, p_head, table, seg, nmt, w_vmem = pl.pallas_call(
            functools.partial(project_kernel, nq, qlen, nd, dlen),
            out_shape=[
                pltpu.VMEM((rows * 8, 128), BF16),
                pltpu.VMEM((nd * dlen, 256), BF16),
                pltpu.VMEM((16, 256), jnp.int32),
                pltpu.VMEM((rows * 8, nq * 8), BF16),
                pltpu.VMEM((dlen, 128), BF16),
                pltpu.VMEM((hidden, 128), BF16),
            ],
            in_specs=[ANY] * 5,
            out_specs=[VMEM] * 6,
            scratch_shapes=[
                pltpu.VMEM((nq * 8, qlen), jnp.int32),
                pltpu.VMEM((rows, hidden), BF16),
                pltpu.VMEM((nd, dlen), jnp.int32),
                pltpu.VMEM((RING, HEAD, hidden), BF16),
                DMA((4,)), DMA((RING,)), DMA((7,)), DMA((7,)), DMA((7,)), DMA((7,)),
            ],
            compiler_params=pltpu.CompilerParams(collective_id=0, has_side_effects=True, vmem_limit_bytes=30 * 2**20),
            name='project',
        )(hbm(query_hidden.reshape(rows, hidden)), hbm(doc_hidden.reshape(nd * dlen, hidden)), hbm(w_proj),
          hbm(query_mask), hbm(doc_mask))

        tail_rows = nd * (dlen - HEAD)
        groups = tail_rows // (GROUP * UNIT)
        best, _ = pl.pallas_call(
            functools.partial(score_kernel, nd, rows, tiles, dlen // UNIT, hidden),
            out_shape=[pltpu.VMEM((tiles, nd, 256), F32), pltpu.VMEM((nd * dlen, 256), BF16)],
            in_specs=[SMEM, VMEM, VMEM, VMEM, VMEM, ANY],
            out_specs=[VMEM, VMEM],
            input_output_aliases={2: 1},
            scratch_shapes=[
                pltpu.VMEM((rows * 8 + 512, 128), F32),
                pltpu.VMEM((tiles + 1, nd, 8, 256), F32),
                pltpu.VMEM((tiles + 1, nd, 8, 256), F32),
                pltpu.VMEM((groups, GROUP * UNIT, hidden), BF16),
                DMA((groups,)),
            ],
            compiler_params=pltpu.CompilerParams(vmem_limit_bytes=36 * 2**20),
            name='score',
        )(table, vmem(q_all), vmem(p_head), vmem(nmt), vmem(w_vmem), hbm(doc_hidden.reshape(nd * dlen, hidden)))

        scores = pl.pallas_call(
            functools.partial(gather_kernel, nd, tiles),
            out_shape=pltpu.VMEM((nd * 8, nq * 8), F32),
            in_specs=[SMEM, VMEM, VMEM],
            out_specs=VMEM,
            scratch_shapes=[DMA((7,)), DMA((7,))],
            compiler_params=pltpu.CompilerParams(collective_id=1, has_side_effects=True),
            name='gather',
        )(temperature.reshape(1), vmem(best), vmem(seg))

        losses, mean = pl.pallas_call(
            functools.partial(loss_kernel, nq),
            out_shape=[jax.ShapeDtypeStruct((1, nq), F32), jax.ShapeDtypeStruct((1, 1), F32)],
            in_specs=[VMEM],
            out_specs=[VMEM, VMEM],
            name='loss',
        )(vmem(scores))
        return losses.reshape(nq), mean.reshape(1)

    tok, mask, row = P(('replica', 'data2', 'data'), None, None), P(('replica', 'data2', 'data'), None), P(('replica', 'data2', 'data'))
    return jax.shard_map(local_step, mesh=mesh, in_specs=(tok, tok, P(None, None), mask, mask, P()),
                         out_specs=(row, P('replica')), check_vma=False)
```
